32 devices in a mesh: gx: 4 (over y, core), gy: 2 (over x), ta: 4 (over z).
Axes of the slice: x: 2, y: 2, z: 4, core: 2. Of those that a mesh axis runs over, the one named last changes fastest.
Arguments:
- link_x: float32 [2, 3, 3, 16, 16, 256], P(None, None, None, 'gx', 'ta', 'gy'), may hold values from -1 to 1, as said below
- link_t: float32 [2, 3, 3, 16, 16, 256], P(None, None, None, 'gx', 'ta', 'gy'), may hold values from -1 to 1, as said below
Outputs:
- loops: float32 [6, 6, 16, 16], P(None, None, 'gx', 'ta')
The draws below stay inside these ranges and needn't reach their ends.
Inputs may be any that keep to these rules, and one draw needn't show every extreme that they name: `link_x`: every link matrix is special unitary. `link_t`: every link matrix is special unitary.
All inputs are finite; a program needn't handle non-finite values.
Results may differ from the reference program's by a relative error of at most 0.0001.
Values sent between devices are 32-bit elements; how exact they have to be, the bound alone decides.
A program may use at most 128 MiB of HBM per device.

```python
import jax
import jax.numpy as jnp

RMAX = 6
TMAX = 6
NX = 16
NT = 16
SPECT = 256


def complex_times(left_mat, right_mat):
    real_rows = []
    imag_rows = []
    for i in range(3):
        real_cols = []
        imag_cols = []
        for k in range(3):
            real_sum = left_mat[0][i][0] * right_mat[0][0][k] - left_mat[1][i][0] * right_mat[1][0][k]
            imag_sum = left_mat[0][i][0] * right_mat[1][0][k] + left_mat[1][i][0] * right_mat[0][0][k]
            for j in range(1, 3):
                real_sum = real_sum + left_mat[0][i][j] * right_mat[0][j][k] - left_mat[1][i][j] * right_mat[1][j][k]
                imag_sum = imag_sum + left_mat[0][i][j] * right_mat[1][j][k] + left_mat[1][i][j] * right_mat[0][j][k]
            real_cols.append(real_sum)
            imag_cols.append(imag_sum)
        real_rows.append(real_cols)
        imag_rows.append(imag_cols)
    return [real_rows, imag_rows]


def embed(theta, phi, psi, first, second):
    ones = jnp.ones_like(theta)
    zeros = jnp.zeros_like(theta)
    real_rows = [[ones if i == k else zeros for k in range(3)] for i in range(3)]
    imag_rows = [[zeros for k in range(3)] for i in range(3)]
    cos_t = jnp.cos(theta)
    sin_t = jnp.sin(theta)
    real_rows[first][first] = cos_t * jnp.cos(phi)
    imag_rows[first][first] = cos_t * jnp.sin(phi)
    real_rows[second][second] = cos_t * jnp.cos(phi)
    imag_rows[second][second] = -cos_t * jnp.sin(phi)
    real_rows[first][second] = sin_t * jnp.cos(psi)
    imag_rows[first][second] = sin_t * jnp.sin(psi)
    real_rows[second][first] = -sin_t * jnp.cos(psi)
    imag_rows[second][first] = sin_t * jnp.sin(psi)
    return [real_rows, imag_rows]


def near_identity(key):
    site_shape = (3, NX, NT, SPECT)
    keys = jax.random.split(key, 3)
    theta = jnp.clip(jax.random.normal(keys[0], site_shape, jnp.float32) * 0.35, -1.2, 1.2)
    phi = jnp.clip(jax.random.normal(keys[1], site_shape, jnp.float32) * 0.35, -1.2, 1.2)
    psi = jax.random.uniform(keys[2], site_shape, jnp.float32, -3.14159265, 3.14159265)
    result = embed(theta[0], phi[0], psi[0], 0, 1)
    result = complex_times(result, embed(theta[1], phi[1], psi[1], 1, 2))
    result = complex_times(result, embed(theta[2], phi[2], psi[2], 0, 2))
    real_part = jnp.stack([jnp.stack(row) for row in result[0]])
    imag_part = jnp.stack([jnp.stack(row) for row in result[1]])
    return jnp.stack([real_part, imag_part])


def draw_link_x(key, part):
    return near_identity(jax.random.fold_in(key, 11))


def draw_link_t(key, part):
    return near_identity(jax.random.fold_in(key, 23))


def setup_inputs(seed: int = 0) -> dict:
    splits = jax.random.split(jax.random.key(seed), 3)
    return {
        "link_x": draw_link_x(jax.random.fold_in(splits[2], 71), 0),
        "link_t": draw_link_t(jax.random.fold_in(splits[2], 71), 0),
    }


def times(left_mat, right_mat):
    real_rows = []
    imag_rows = []
    for i in range(3):
        real_cols = []
        imag_cols = []
        for k in range(3):
            real_sum = left_mat[0, i, 0] * right_mat[0, 0, k] - left_mat[1, i, 0] * right_mat[1, 0, k]
            imag_sum = left_mat[0, i, 0] * right_mat[1, 0, k] + left_mat[1, i, 0] * right_mat[0, 0, k]
            for j in range(1, 3):
                real_sum = real_sum + left_mat[0, i, j] * right_mat[0, j, k] - left_mat[1, i, j] * right_mat[1, j, k]
                imag_sum = imag_sum + left_mat[0, i, j] * right_mat[1, j, k] + left_mat[1, i, j] * right_mat[0, j, k]
            real_cols.append(real_sum)
            imag_cols.append(imag_sum)
        real_rows.append(jnp.stack(real_cols))
        imag_rows.append(jnp.stack(imag_cols))
    return jnp.stack([jnp.stack(real_rows), jnp.stack(imag_rows)])


def correlation(upper_half, lower_half):
    return jnp.sum(upper_half * lower_half, axis=(0, 1, 2, 5))


def reference(link_x, link_t):
    temporal = [link_t]
    factor = link_t
    for extent in range(1, TMAX):
        factor = jnp.roll(factor, -1, axis=4)
        temporal.append(times(temporal[-1], factor))
    carried = list(temporal)
    spatial = link_x
    factor_x = link_x
    all_rows = []
    for radius in range(RMAX):
        if radius > 0:
            factor_x = jnp.roll(factor_x, -1, axis=3)
            spatial = times(spatial, factor_x)
        carried = [jnp.roll(field, -1, axis=3) for field in carried]
        shifted = spatial
        row_sums = []
        for extent in range(TMAX):
            shifted = jnp.roll(shifted, -1, axis=4)
            upper_half = times(spatial, carried[extent])
            lower_half = times(temporal[extent], shifted)
            row_sums.append(correlation(upper_half, lower_half))
        all_rows.append(jnp.stack(row_sums))
    return jnp.stack(all_rows) / (3.0 * SPECT)
```

```python
import functools

import jax
import jax.numpy as jnp
from jax import lax
from jax.experimental import pallas as pl
from jax.experimental.pallas import tpu as pltpu
from jax.sharding import PartitionSpec as P

RMAX = 6
TMAX = 6
LANES = 128
ROWS = 8
MESH = pl.DeviceIdType.MESH


def product(left, right):
    (ar, ai), (br, bi) = left, right
    real = imag = None
    for j in range(3):
        a_re, a_im = ar[:, j][:, None], ai[:, j][:, None]
        b_re, b_im = br[j][None], bi[j][None]
        re = a_re * b_re - a_im * b_im
        im = a_re * b_im + a_im * b_re
        real = re if real is None else real + re
        imag = im if imag is None else imag + im
    return real, imag


def product_dagger(left, right):
    (ar, ai), (br, bi) = left, right
    real = imag = None
    for j in range(3):
        a_re, a_im = ar[:, j][:, None], ai[:, j][:, None]
        b_re, b_im = br[:, j][None], bi[:, j][None]
        re = a_re * b_re + a_im * b_im
        im = a_im * b_re - a_re * b_im
        real = re if real is None else real + re
        imag = im if imag is None else imag + im
    return real, imag


def load(ref, start):
    block = ref[:, pl.ds(start, ROWS), :]
    block = block.reshape(2, 3, 3, ROWS, LANES)
    return block[0], block[1]


def store(ref, start, mat):
    ref[0:9, pl.ds(start, ROWS), :] = mat[0].reshape(9, ROWS, LANES)
    ref[9:18, pl.ds(start, ROWS), :] = mat[1].reshape(9, ROWS, LANES)


def complete(two_rows):
    re = two_rows[0:6].reshape(2, 3, ROWS, LANES)
    im = two_rows[6:12].reshape(2, 3, ROWS, LANES)
    third_re, third_im = [], []
    for k in range(3):
        p, q = (k + 1) % 3, (k + 2) % 3
        third_re.append(
            re[0, p] * re[1, q] - im[0, p] * im[1, q] - re[0, q] * re[1, p] + im[0, q] * im[1, p]
        )
        third_im.append(
            re[0, q] * im[1, p] + im[0, q] * re[1, p] - re[0, p] * im[1, q] - im[0, p] * re[1, q]
        )
    real = jnp.concatenate([re, jnp.stack(third_re)[None]], axis=0)
    imag = jnp.concatenate([im, jnp.stack(third_im)[None]], axis=0)
    return real, imag


def spread(total, nx, nt, sub, out_ref):
    shape = (nx * nt, LANES)
    corner = lax.broadcasted_iota(jnp.int32, shape, 0)
    column = lax.broadcasted_iota(jnp.int32, shape, 1)
    base = (corner % nt) * (nx * sub) + (corner // nt) * sub
    for r in range(RMAX):
        first = r * TMAX // sub
        item = jnp.minimum(column + (r * TMAX - first * sub), 2 * sub - 1)
        lanes = base + item % sub
        value = None
        for g in range(first, (r * TMAX + TMAX - 1) // sub + 1):
            line = jnp.broadcast_to(total[g : g + 1], shape)
            line = jnp.take_along_axis(line, lanes, axis=1)
            value = line if value is None else jnp.where(item < sub, value, line)
        out_ref[r] = value.reshape(nx, nt, LANES)[:, :, :TMAX]


def kernel(
    dims, lx_ref, lt_ref, out_ref, raw, send, recv, links, pref, trans, part, gath,
    in_sem, own_sem, send_sem, recv_sem, send2_sem, recv2_sem,
):
    gx, gy, ta, nx, nt, ns, sub = dims
    groups = gx * ta
    total_t = ta * nt
    mx, my, mt = lax.axis_index("gx"), lax.axis_index("gy"), lax.axis_index("ta")
    me = mt * gx + mx
    comps = 24
    sites = nx * nt

    loads = []
    for f, ref in enumerate((lx_ref, lt_ref)):
        for c in range(2):
            q = f * 2 + c
            loads.append(
                pltpu.make_async_copy(
                    ref.at[c, pl.ds(0, 6 * sites)],
                    raw.at[pl.ds(q * 6 * sites, 6 * sites)],
                    in_sem.at[q],
                )
            )
            loads[-1].start()

    offsets = [(a, b, c) for c in range(ta) for b in range(gy) for a in range(gx)]
    offsets = [o for o in reversed(offsets) if o != (0, 0, 0)]

    def target(offset):
        a, b, c = offset
        return {
            "gx": lax.rem(mx + a, gx),
            "gy": lax.rem(my + b, gy),
            "ta": lax.rem(mt + c, ta),
        }

    barrier = pltpu.get_barrier_semaphore()
    for offset in offsets:
        pl.semaphore_signal(barrier, inc=1, device_id=target(offset), device_id_type=MESH)

    for copy in loads:
        copy.wait()
    width = nt * comps
    spare = LANES - width

    def layer(x):
        rows = [raw[pl.ds(x * nt + t, comps, stride=sites), :] for t in range(nt)]
        return jnp.concatenate(rows, axis=0)

    last = layer(nx - 1)
    for x in range(nx - 1):
        turned = jnp.concatenate([layer(x), last[x * spare : (x + 1) * spare]], axis=0).T
        send[:, pl.ds(x * sub, sub), :] = turned.reshape(groups, sub, LANES)

    pl.semaphore_wait(barrier, len(offsets))

    plane = [o for o in offsets if o[1] == 0]
    copies = []
    for k, offset in enumerate(plane):
        where = target(offset)
        copies.append(
            pltpu.make_async_remote_copy(
                src_ref=send.at[where["ta"] * gx + where["gx"]],
                dst_ref=recv.at[me],
                send_sem=send_sem.at[k],
                recv_sem=recv_sem.at[k],
                device_id=where,
                device_id_type=MESH,
            )
        )
        copies[-1].start()
    own = pltpu.make_async_copy(send.at[me], recv.at[me], own_sem.at[0])
    own.start()
    own.wait()

    lane_x = lax.broadcasted_iota(jnp.int32, (width, LANES), 1) // sub % nx
    for c in range(ta):
        for copy, offset in zip(copies, plane):
            if offset[2] == c:
                copy.wait()
        t_dev = lax.rem(mt + ta - c, ta)
        block = recv[pl.ds(t_dev * gx, gx)]
        block = jnp.concatenate([block, jnp.zeros((gx, sub, LANES), jnp.float32)], axis=1)
        block = block.reshape(LANES, LANES).T
        rest = [pltpu.roll(block[width:], (nx - 1 - x) * sub, 1) for x in range(nx - 1)]
        block = jnp.where(lane_x == nx - 1, jnp.concatenate(rest, axis=0), block[:width])
        for t in range(nt):
            links[:, t_dev * nt + t, :] = block[t * comps : (t + 1) * comps]

    for e in range(18):
        value = 1.0 if e in (0, 4, 8) else 0.0
        pref[e, 0:ROWS, :] = jnp.full((ROWS, LANES), value, jnp.float32)
    for start in range(0, total_t, ROWS):
        store(pref, ROWS + start, complete(links[12:24, pl.ds(start, ROWS), :]))
    step = 1
    while step < total_t:
        for start in reversed(range(0, total_t, ROWS)):
            if start + ROWS > step:
                earlier = load(pref, ROWS + start - step)
                store(pref, ROWS + start, product(earlier, load(pref, ROWS + start)))
        step *= 2
    loop = pref[:, total_t + ROWS - 1 : total_t + ROWS, :].reshape(2, 3, 3, 1, LANES)
    loop = jnp.broadcast_to(loop, (2, 3, 3, ROWS, LANES))
    store(pref, ROWS + total_t, product((loop[0], loop[1]), load(pref, ROWS)))

    def next_x(mat):
        return tuple(
            pltpu.roll(m.reshape(9 * ROWS, LANES), LANES - sub, 1).reshape(3, 3, ROWS, LANES)
            for m in mat
        )

    for start in range(0, total_t + ROWS, ROWS):
        gauge = load(pref, ROWS - 1 + start)
        link = complete(links[0:12, pl.ds(start % total_t, ROWS), :])
        moved = product_dagger(product(gauge, link), next_x(gauge))
        store(trans.at[0], start, moved)
        path = moved
        for r in range(1, RMAX):
            moved = next_x(moved)
            path = product(path, moved)
            store(trans.at[r], start, path)

    lane = lax.broadcasted_iota(jnp.int32, (total_t, LANES), 1)
    row = lax.broadcasted_iota(jnp.int32, (total_t, LANES), 0)
    sums = []
    for r in range(RMAX):
        for u in range(1, TMAX + 1):
            halves = []
            for start in range(0, total_t, ROWS):
                here = trans[r, :, pl.ds(start, ROWS), :]
                there = trans[r, :, pl.ds(start + u, ROWS), :]
                halves.append(jnp.sum(here * there, axis=0))
            sums.append(jnp.concatenate(halves, axis=0))

    def merge(items, width):
        if width == 0:
            return items[0]
        half = width
        low = [i for i in items[:half]]
        high = [i for i in items[half:]]
        first = merge(low, width // 2)
        first = first + pltpu.roll(first, LANES - width, 1)
        if not high:
            return first
        second = merge(high, width // 2)
        second = second + pltpu.roll(second, width, 1)
        return jnp.where((lane & width) == 0, first, second)

    def fold(items):
        return merge(items, sub // 2)

    block = LANES // gx
    for g in range(-(-len(sums) // sub)):
        value = fold(sums[g * sub : (g + 1) * sub])
        bit = 1
        while bit < gx:
            i_bit = (row & bit) != 0
            j_bit = ((lane // block) & bit) != 0
            up = pltpu.roll(pltpu.roll(value, total_t - bit, 0), block * bit, 1)
            down = pltpu.roll(pltpu.roll(value, bit, 0), LANES - block * bit, 1)
            value = jnp.where(i_bit == j_bit, value, jnp.where(j_bit, up, down))
            bit *= 2
        part[:, g, :] = value

    slot = my * groups + me
    copies2 = []
    for k, offset in enumerate(offsets):
        where = target(offset)
        copies2.append(
            pltpu.make_async_remote_copy(
                src_ref=part.at[where["ta"] * gx + where["gx"]],
                dst_ref=gath.at[slot],
                send_sem=send2_sem.at[k],
                recv_sem=recv2_sem.at[k],
                device_id=where,
                device_id_type=MESH,
            )
        )
        copies2[-1].start()
    own2 = pltpu.make_async_copy(part.at[me], gath.at[slot], own_sem.at[1])
    own2.start()
    own2.wait()
    for copy in copies2:
        copy.wait()
    spread(jnp.sum(gath[...], axis=0) / (3.0 * (ns * gy)), nx, nt, sub, out_ref)


def fast(dims, link_x, link_t):
    gx, gy, ta, nx, nt, ns, sub = dims
    groups = gx * ta
    total_t = ta * nt
    flat = (2, 9 * nx * nt, ns)
    rows = -(-RMAX * TMAX // sub)
    out = pl.pallas_call(
        functools.partial(kernel, dims),
        out_shape=pltpu.VMEM((RMAX, nx, nt, TMAX), jnp.float32),
        in_specs=[pl.BlockSpec(memory_space=pl.ANY)] * 2,
        out_specs=pl.BlockSpec(memory_space=pltpu.VMEM),
        scratch_shapes=[
            pltpu.VMEM((24 * nx * nt, ns), jnp.float32),
            pltpu.VMEM((groups, (nx - 1) * sub, LANES), jnp.float32),
            pltpu.VMEM((groups, (nx - 1) * sub, LANES), jnp.float32),
            pltpu.VMEM((24, total_t, LANES), jnp.float32),
            pltpu.VMEM((18, total_t + 2 * ROWS, LANES), jnp.float32),
            pltpu.VMEM((RMAX, 18, total_t + ROWS, LANES), jnp.float32),
            pltpu.VMEM((groups, rows, LANES), jnp.float32),
            pltpu.VMEM((gy * groups, rows, LANES), jnp.float32),
            pltpu.SemaphoreType.DMA((4,)),
            pltpu.SemaphoreType.DMA((2,)),
            pltpu.SemaphoreType.DMA((groups - 1,)),
            pltpu.SemaphoreType.DMA((groups - 1,)),
            pltpu.SemaphoreType.DMA((gy * groups - 1,)),
            pltpu.SemaphoreType.DMA((gy * groups - 1,)),
        ],
        compiler_params=pltpu.CompilerParams(collective_id=0, has_side_effects=True),
        name="wilson",
    )(link_x.reshape(flat), link_t.reshape(flat))
    return out.transpose(0, 3, 1, 2)


def times(left, right):
    def dot(a, b):
        return sum(a[:, j][:, None] * b[j][None] for j in range(3))

    real = dot(left[0], right[0]) - dot(left[1], right[1])
    imag = dot(left[0], right[1]) + dot(left[1], right[0])
    return jnp.stack([real, imag])


def general(dims, link_x, link_t):
    gx, gy, ta, nx, nt, ns, sub = dims

    def gather(field):
        field = lax.all_to_all(field, "gx", 5, 3, tiled=True)
        return lax.all_to_all(field, "ta", 5, 4, tiled=True)

    link_x, link_t = gather(link_x), gather(link_t)

    def grow_t(carry, _):
        line, factor = carry
        factor = jnp.roll(factor, -1, axis=4)
        return (times(line, factor), factor), line

    _, temporal = lax.scan(grow_t, (link_t, link_t), None, length=TMAX)

    def radius(carry, _):
        spatial, factor, carried = carry
        carried = jnp.roll(carried, -1, axis=4)

        def extent(shifted, pair):
            line, line_r = pair
            shifted = jnp.roll(shifted, -1, axis=4)
            return shifted, jnp.sum(times(spatial, line_r) * times(line, shifted), axis=(0, 1, 2, 5))

        _, sums = lax.scan(extent, spatial, (temporal, carried))
        factor = jnp.roll(factor, -1, axis=3)
        return (times(spatial, factor), factor, carried), sums

    _, loops = lax.scan(radius, (link_x, link_x, temporal), None, length=RMAX)
    loops = lax.psum(loops, ("gx", "gy", "ta"))
    loops = lax.dynamic_slice_in_dim(loops, lax.axis_index("gx") * nx, nx, axis=2)
    loops = lax.dynamic_slice_in_dim(loops, lax.axis_index("ta") * nt, nt, axis=3)
    return loops / (3.0 * (ns * gy))


def local(link_x, link_t):
    gx, gy, ta = (lax.axis_size(a) for a in ("gx", "gy", "ta"))
    nx, nt, ns = link_x.shape[3:]
    sub = ns // (gx * ta)
    dims = (gx, gy, ta, nx, nt, ns, sub)
    fits = (
        ns == LANES
        and sub == ROWS
        and gx * nx * sub == LANES
        and nt == gx
        and gx & (gx - 1) == 0
        and nt * 24 < LANES
        and nt * 24 == (nx - 1) * (LANES - nt * 24)
        and (ta * nt) % ROWS == 0
        and ta * nt >= TMAX
    )
    return (fast if fits else general)(dims, link_x, link_t)


def solution(mesh):
    spec = P(None, None, None, "gx", "ta", "gy")
    return jax.shard_map(
        local,
        mesh=mesh,
        in_specs=(spec, spec),
        out_specs=P(None, None, "gx", "ta"),
        check_vma=False,
    )
```

```python
import functools

import jax
import jax.numpy as jnp
from jax import lax
from jax.experimental import pallas as pl
from jax.experimental.pallas import tpu as pltpu
from jax.sharding import PartitionSpec as P

RMAX = 6
TMAX = 6
LANES = 128
ROWS = 8
MESH = pl.DeviceIdType.MESH


def product(left, right):
    (ar, ai), (br, bi) = left, right
    real = imag = None
    for j in range(3):
        a_re, a_im = ar[:, j][:, None], ai[:, j][:, None]
        b_re, b_im = br[j][None], bi[j][None]
        re = a_re * b_re - a_im * b_im
        im = a_re * b_im + a_im * b_re
        real = re if real is None else real + re
        imag = im if imag is None else imag + im
    return real, imag


def product_dagger(left, right):
    (ar, ai), (br, bi) = left, right
    real = imag = None
    for j in range(3):
        a_re, a_im = ar[:, j][:, None], ai[:, j][:, None]
        b_re, b_im = br[:, j][None], bi[:, j][None]
        re = a_re * b_re + a_im * b_im
        im = a_im * b_re - a_re * b_im
        real = re if real is None else real + re
        imag = im if imag is None else imag + im
    return real, imag


def load(ref, start):
    block = ref[:, pl.ds(start, ROWS), :]
    block = block.reshape(2, 3, 3, ROWS, LANES)
    return block[0], block[1]


def store(ref, start, mat):
    ref[0:9, pl.ds(start, ROWS), :] = mat[0].reshape(9, ROWS, LANES)
    ref[9:18, pl.ds(start, ROWS), :] = mat[1].reshape(9, ROWS, LANES)


def complete(two_rows):
    re = two_rows[0:6].reshape(2, 3, ROWS, LANES)
    im = two_rows[6:12].reshape(2, 3, ROWS, LANES)
    third_re, third_im = [], []
    for k in range(3):
        p, q = (k + 1) % 3, (k + 2) % 3
        third_re.append(
            re[0, p] * re[1, q] - im[0, p] * im[1, q] - re[0, q] * re[1, p] + im[0, q] * im[1, p]
        )
        third_im.append(
            re[0, q] * im[1, p] + im[0, q] * re[1, p] - re[0, p] * im[1, q] - im[0, p] * re[1, q]
        )
    real = jnp.concatenate([re, jnp.stack(third_re)[None]], axis=0)
    imag = jnp.concatenate([im, jnp.stack(third_im)[None]], axis=0)
    return real, imag


def spread(total, nx, nt, sub, out_ref):
    shape = (nx * nt, LANES)
    corner = lax.broadcasted_iota(jnp.int32, shape, 0)
    column = lax.broadcasted_iota(jnp.int32, shape, 1)
    base = (corner % nt) * (nx * sub) + (corner // nt) * sub
    for r in range(RMAX):
        first = r * TMAX // sub
        item = jnp.minimum(column + (r * TMAX - first * sub), 2 * sub - 1)
        lanes = base + item % sub
        value = None
        for g in range(first, (r * TMAX + TMAX - 1) // sub + 1):
            line = jnp.broadcast_to(total[g : g + 1], shape)
            line = jnp.take_along_axis(line, lanes, axis=1)
            value = line if value is None else jnp.where(item < sub, value, line)
        out_ref[r] = value.reshape(nx, nt, LANES)[:, :, :TMAX]


def kernel(
    dims, lx_ref, lt_ref, out_ref, raw, send, recv, links, pref, trans, part, gath,
    in_sem, send_sem, recv_sem, send2_sem, recv2_sem, entered,
):
    gx, gy, ta, nx, nt, ns, sub = dims
    groups = gx * ta
    total_t = ta * nt
    mx, my, mt = lax.axis_index("gx"), lax.axis_index("gy"), lax.axis_index("ta")
    me = mt * gx + mx
    comps = 24
    sites = nx * nt

    loads = []
    for f, ref in enumerate((lx_ref, lt_ref)):
        for c in range(2):
            q = f * 2 + c
            loads.append(
                pltpu.make_async_copy(
                    ref.at[c, pl.ds(0, 6 * sites)],
                    raw.at[pl.ds(q * 6 * sites, 6 * sites)],
                    in_sem,
                )
            )
            loads[-1].start()

    offsets = [(a, b, c) for c in range(ta) for b in range(gy) for a in range(gx)]
    offsets = [o for o in reversed(offsets) if o != (0, 0, 0)]

    def target(offset):
        a, b, c = offset
        return {
            "gx": lax.rem(mx + a, gx),
            "gy": lax.rem(my + b, gy),
            "ta": lax.rem(mt + c, ta),
        }

    plane = [o for o in offsets if o[1] == 0]
    peers = [o for o in offsets if o[0] == 0 and o[2] == 0]
    barrier = pltpu.get_barrier_semaphore()
    for offset in plane + peers:
        pl.semaphore_signal(barrier, inc=1, device_id=target(offset), device_id_type=MESH)

    pltpu.make_async_copy(raw, raw, in_sem).wait()
    width = nt * comps
    spare = LANES - width

    def layer(x):
        rows = [raw[pl.ds(x * nt + t, comps, stride=sites), :] for t in range(nt)]
        return jnp.concatenate(rows, axis=0)

    last = layer(nx - 1)
    for x in range(nx - 1):
        turned = jnp.concatenate([layer(x), last[x * spare : (x + 1) * spare]], axis=0).T
        send[:, pl.ds(x * sub, sub), :] = turned.reshape(groups, sub, LANES)

    pl.semaphore_wait(barrier, len(plane + peers))
    for offset in peers:
        pl.semaphore_signal(entered, inc=1, device_id=target(offset), device_id_type=MESH)

    copies = []
    for k, offset in enumerate(plane):
        where = target(offset)
        copies.append(
            pltpu.make_async_remote_copy(
                src_ref=send.at[where["ta"] * gx + where["gx"]],
                dst_ref=recv.at[me],
                send_sem=send_sem,
                recv_sem=recv_sem.at[offset[2]],
                device_id=where,
                device_id_type=MESH,
            )
        )
        copies[-1].start()
    recv[pl.ds(me, 1)] = send[pl.ds(me, 1)]

    lane_x = lax.broadcasted_iota(jnp.int32, (width, LANES), 1) // sub % nx
    for c in range(ta):
        landed = recv.at[pl.ds(0, gx if c else gx - 1)]
        pltpu.make_async_copy(landed, landed, recv_sem.at[c]).wait()
        t_dev = lax.rem(mt + ta - c, ta)
        block = recv[pl.ds(t_dev * gx, gx)]
        block = jnp.concatenate([block, jnp.zeros((gx, sub, LANES), jnp.float32)], axis=1)
        block = block.reshape(LANES, LANES).T
        rest = [pltpu.roll(block[width:], (nx - 1 - x) * sub, 1) for x in range(nx - 1)]
        block = jnp.where(lane_x == nx - 1, jnp.concatenate(rest, axis=0), block[:width])
        for t in range(nt):
            links[:, t_dev * nt + t, :] = block[t * comps : (t + 1) * comps]

    for e in range(18):
        value = 1.0 if e in (0, 4, 8) else 0.0
        pref[e, 0:ROWS, :] = jnp.full((ROWS, LANES), value, jnp.float32)
    for start in range(0, total_t, ROWS):
        store(pref, ROWS + start, complete(links[12:24, pl.ds(start, ROWS), :]))
    step = 1
    while step < total_t:
        for start in reversed(range(0, total_t, ROWS)):
            if start + ROWS > step:
                earlier = load(pref, ROWS + start - step)
                store(pref, ROWS + start, product(earlier, load(pref, ROWS + start)))
        step *= 2
    loop = pref[:, total_t + ROWS - 1 : total_t + ROWS, :].reshape(2, 3, 3, 1, LANES)
    loop = jnp.broadcast_to(loop, (2, 3, 3, ROWS, LANES))
    store(pref, ROWS + total_t, product((loop[0], loop[1]), load(pref, ROWS)))

    def next_x(mat):
        return tuple(
            pltpu.roll(m.reshape(9 * ROWS, LANES), LANES - sub, 1).reshape(3, 3, ROWS, LANES)
            for m in mat
        )

    for start in range(0, total_t + ROWS, ROWS):
        gauge = load(pref, ROWS - 1 + start)
        link = complete(links[0:12, pl.ds(start % total_t, ROWS), :])
        moved = product_dagger(product(gauge, link), next_x(gauge))
        store(trans.at[0], start, moved)
        path = moved
        for r in range(1, RMAX):
            moved = next_x(moved)
            path = product(path, moved)
            store(trans.at[r], start, path)

    lane = lax.broadcasted_iota(jnp.int32, (total_t, LANES), 1)
    row = lax.broadcasted_iota(jnp.int32, (total_t, LANES), 0)
    sums = []
    for r in range(RMAX):
        for u in range(1, TMAX + 1):
            halves = []
            for start in range(0, total_t, ROWS):
                here = trans[r, :, pl.ds(start, ROWS), :]
                there = trans[r, :, pl.ds(start + u, ROWS), :]
                halves.append(jnp.sum(here * there, axis=0))
            sums.append(jnp.concatenate(halves, axis=0))

    def merge(items, width):
        if width == 0:
            return items[0]
        half = width
        low = [i for i in items[:half]]
        high = [i for i in items[half:]]
        first = merge(low, width // 2)
        first = first + pltpu.roll(first, LANES - width, 1)
        if not high:
            return first
        second = merge(high, width // 2)
        second = second + pltpu.roll(second, width, 1)
        return jnp.where((lane & width) == 0, first, second)

    def fold(items):
        return merge(items, sub // 2)

    block = LANES // gx
    for g in range(-(-len(sums) // sub)):
        value = fold(sums[g * sub : (g + 1) * sub])
        bit = 1
        while bit < gx:
            i_bit = (row & bit) != 0
            j_bit = ((lane // block) & bit) != 0
            up = pltpu.roll(pltpu.roll(value, total_t - bit, 0), block * bit, 1)
            down = pltpu.roll(pltpu.roll(value, bit, 0), LANES - block * bit, 1)
            value = jnp.where(i_bit == j_bit, value, jnp.where(j_bit, up, down))
            bit *= 2
        part[:, g, :] = value

    slot = my * groups + me
    pl.semaphore_wait(entered, len(peers))
    copies2 = []
    for k, offset in enumerate(offsets):
        where = target(offset)
        copies2.append(
            pltpu.make_async_remote_copy(
                src_ref=part.at[where["ta"] * gx + where["gx"]],
                dst_ref=gath.at[slot],
                send_sem=send2_sem,
                recv_sem=recv2_sem,
                device_id=where,
                device_id_type=MESH,
            )
        )
        copies2[-1].start()
    gath[pl.ds(slot, 1)] = part[pl.ds(me, 1)]
    sent = send.at[pl.ds(0, len(plane))]
    pltpu.make_async_copy(sent, sent, send_sem).wait()
    landed = gath.at[pl.ds(0, len(offsets))]
    pltpu.make_async_copy(landed, landed, send2_sem).wait()
    pltpu.make_async_copy(landed, landed, recv2_sem).wait()
    spread(jnp.sum(gath[...], axis=0) / (3.0 * (ns * gy)), nx, nt, sub, out_ref)


def fast(dims, link_x, link_t):
    gx, gy, ta, nx, nt, ns, sub = dims
    groups = gx * ta
    total_t = ta * nt
    flat = (2, 9 * nx * nt, ns)
    rows = -(-RMAX * TMAX // sub)
    out = pl.pallas_call(
        functools.partial(kernel, dims),
        out_shape=pltpu.VMEM((RMAX, nx, nt, TMAX), jnp.float32),
        in_specs=[pl.BlockSpec(memory_space=pl.ANY)] * 2,
        out_specs=pl.BlockSpec(memory_space=pltpu.VMEM),
        scratch_shapes=[
            pltpu.VMEM((24 * nx * nt, ns), jnp.float32),
            pltpu.VMEM((groups, (nx - 1) * sub, LANES), jnp.float32),
            pltpu.VMEM((groups, (nx - 1) * sub, LANES), jnp.float32),
            pltpu.VMEM((24, total_t, LANES), jnp.float32),
            pltpu.VMEM((18, total_t + 2 * ROWS, LANES), jnp.float32),
            pltpu.VMEM((RMAX, 18, total_t + ROWS, LANES), jnp.float32),
            pltpu.VMEM((groups, rows, LANES), jnp.float32),
            pltpu.VMEM((gy * groups, rows, LANES), jnp.float32),
            pltpu.SemaphoreType.DMA,
            pltpu.SemaphoreType.DMA,
            pltpu.SemaphoreType.DMA((ta,)),
            pltpu.SemaphoreType.DMA,
            pltpu.SemaphoreType.DMA,
            pltpu.SemaphoreType.REGULAR,
        ],
        compiler_params=pltpu.CompilerParams(collective_id=0, has_side_effects=True),
        name="wilson",
    )(link_x.reshape(flat), link_t.reshape(flat))
    return out.transpose(0, 3, 1, 2)


def times(left, right):
    def dot(a, b):
        return sum(a[:, j][:, None] * b[j][None] for j in range(3))

    real = dot(left[0], right[0]) - dot(left[1], right[1])
    imag = dot(left[0], right[1]) + dot(left[1], right[0])
    return jnp.stack([real, imag])


def general(dims, link_x, link_t):
    gx, gy, ta, nx, nt, ns, sub = dims

    def gather(field):
        field = lax.all_to_all(field, "gx", 5, 3, tiled=True)
        return lax.all_to_all(field, "ta", 5, 4, tiled=True)

    link_x, link_t = gather(link_x), gather(link_t)

    def grow_t(carry, _):
        line, factor = carry
        factor = jnp.roll(factor, -1, axis=4)
        return (times(line, factor), factor), line

    _, temporal = lax.scan(grow_t, (link_t, link_t), None, length=TMAX)

    def radius(carry, _):
        spatial, factor, carried = carry
        carried = jnp.roll(carried, -1, axis=4)

        def extent(shifted, pair):
            line, line_r = pair
            shifted = jnp.roll(shifted, -1, axis=4)
            return shifted, jnp.sum(times(spatial, line_r) * times(line, shifted), axis=(0, 1, 2, 5))

        _, sums = lax.scan(extent, spatial, (temporal, carried))
        factor = jnp.roll(factor, -1, axis=3)
        return (times(spatial, factor), factor, carried), sums

    _, loops = lax.scan(radius, (link_x, link_x, temporal), None, length=RMAX)
    loops = lax.psum(loops, ("gx", "gy", "ta"))
    loops = lax.dynamic_slice_in_dim(loops, lax.axis_index("gx") * nx, nx, axis=2)
    loops = lax.dynamic_slice_in_dim(loops, lax.axis_index("ta") * nt, nt, axis=3)
    return loops / (3.0 * (ns * gy))


def local(link_x, link_t):
    gx, gy, ta = (lax.axis_size(a) for a in ("gx", "gy", "ta"))
    nx, nt, ns = link_x.shape[3:]
    sub = ns // (gx * ta)
    dims = (gx, gy, ta, nx, nt, ns, sub)
    fits = (
        ns == LANES
        and sub == ROWS
        and gx * nx * sub == LANES
        and nt == gx
        and gx & (gx - 1) == 0
        and nt * 24 < LANES
        and nt * 24 == (nx - 1) * (LANES - nt * 24)
        and (ta * nt) % ROWS == 0
        and ta * nt >= TMAX
    )
    return (fast if fits else general)(dims, link_x, link_t)


def solution(mesh):
    spec = P(None, None, None, "gx", "ta", "gy")
    return jax.shard_map(
        local,
        mesh=mesh,
        in_specs=(spec, spec),
        out_specs=P(None, None, "gx", "ta"),
        check_vma=False,
    )
```

```python
import contextlib
import functools

import jax
import jax.numpy as jnp
from jax import lax
from jax.experimental import pallas as pl
from jax.experimental.pallas import tpu as pltpu
from jax.sharding import PartitionSpec as P

RMAX = 6
TMAX = 6
LANES = 128
ROWS = 8
MESH = pl.DeviceIdType.MESH
scope = lambda name: contextlib.nullcontext()


def product(left, right):
    (ar, ai), (br, bi) = left, right
    real = imag = None
    for j in range(3):
        a_re, a_im = ar[:, j][:, None], ai[:, j][:, None]
        b_re, b_im = br[j][None], bi[j][None]
        re = a_re * b_re - a_im * b_im
        im = a_re * b_im + a_im * b_re
        real = re if real is None else real + re
        imag = im if imag is None else imag + im
    return real, imag


def product_dagger(left, right):
    (ar, ai), (br, bi) = left, right
    real = imag = None
    for j in range(3):
        a_re, a_im = ar[:, j][:, None], ai[:, j][:, None]
        b_re, b_im = br[:, j][None], bi[:, j][None]
        re = a_re * b_re + a_im * b_im
        im = a_im * b_re - a_re * b_im
        real = re if real is None else real + re
        imag = im if imag is None else imag + im
    return real, imag


def third(two):
    (ar, br), (ai, bi) = ((m[0], m[1]) for m in two)
    real, imag = [], []
    for k in range(3):
        p, q = (k + 1) % 3, (k + 2) % 3
        real.append(ar[p] * br[q] - ai[p] * bi[q] - ar[q] * br[p] + ai[q] * bi[p])
        imag.append(ar[q] * bi[p] + ai[q] * br[p] - ar[p] * bi[q] - ai[p] * br[q])
    return jnp.stack(real), jnp.stack(imag)


def full(two):
    return tuple(jnp.concatenate([m, t[None]], axis=0) for m, t in zip(two, third(two)))


def unit_where(mask, mat):
    rows = mat[0].shape[0]
    real = [
        jnp.stack([jnp.where(mask, mat[0][i, k], 1.0 if i == k else 0.0) for k in range(3)])
        for i in range(rows)
    ]
    return jnp.stack(real), jnp.where(mask, mat[1], 0.0)


def rolled(mat, shift, axis):
    return tuple(
        pltpu.roll(m.reshape(-1, *m.shape[2:]), shift, axis).reshape(m.shape) for m in mat
    )


def pivot(mat):
    size = [jnp.maximum(jnp.abs(mat[0][0, k]), jnp.abs(mat[1][0, k])) for k in range(3)]
    first = (size[0] >= size[1]) & (size[0] >= size[2])
    return first, size[1] >= size[2]


def choose(masks, a, b, c):
    return jnp.where(masks[0], a, jnp.where(masks[1], b, c))


def shorten(mat):
    masks = pivot(mat)
    parts = [m[0, k] for m in mat for k in range(3)]
    for m in mat:
        b = m[1]
        parts.append(choose(masks, b[1], b[2], b[0]))
        parts.append(choose(masks, b[2], b[0], b[1]))
    return parts


def lengthen(parts):
    ar, ai = parts[0:3], parts[3:6]
    (pr, qr), (pi, qi) = parts[6:8], parts[8:10]
    masks = pivot((parts[None, 0:3], parts[None, 3:6]))
    cr, ci = (choose(masks, a[0], a[1], a[2]) for a in (ar, ai))
    dr, di = (choose(masks, a[1], a[2], a[0]) for a in (ar, ai))
    er, ei = (choose(masks, a[2], a[0], a[1]) for a in (ar, ai))
    wr = dr * pr + di * pi + er * qr + ei * qi
    wi = dr * pi - di * pr + er * qi - ei * qr
    scale = -1.0 / (cr * cr + ci * ci)
    kr, ki = (wr * cr - wi * ci) * scale, (wr * ci + wi * cr) * scale
    second = []
    for k, p, q in ((kr, pr, qr), (ki, pi, qi)):
        second.append(jnp.stack([choose(masks, k, q, p), choose(masks, p, k, q), choose(masks, q, p, k)]))
    return jnp.stack([ar, second[0]]), jnp.stack([ai, second[1]])


def pair(block):
    half = block.reshape(2, -1, *block.shape[1:])
    return tuple(m.reshape(-1, 3, *block.shape[1:]) for m in half)


def flat(mat):
    return jnp.concatenate([m.reshape(-1, *m.shape[2:]) for m in mat], axis=0)


def swap(block, sub):
    row = lax.broadcasted_iota(jnp.int32, block.shape, 1) // (ROWS // 2)
    lane = lax.broadcasted_iota(jnp.int32, block.shape, 2) // sub % 2
    turned = pltpu.roll(block, ROWS // 2, 1)
    up, down = pltpu.roll(turned, sub, 2), pltpu.roll(turned, LANES - sub, 2)
    return jnp.where(row == lane, block, jnp.where(lane == 1, up, down))


def spread(total, nx, nt, sub, out_ref):
    shape = (nx * nt, LANES)
    corner = lax.broadcasted_iota(jnp.int32, shape, 0)
    column = lax.broadcasted_iota(jnp.int32, shape, 1)
    base = (corner % nt) * (nx * sub) + (corner // nt) * sub
    for r in range(RMAX):
        first = r * TMAX // sub
        item = jnp.minimum(column + (r * TMAX - first * sub), 2 * sub - 1)
        lanes = base + item % sub
        value = None
        for g in range(first, (r * TMAX + TMAX - 1) // sub + 1):
            line = jnp.broadcast_to(total[g : g + 1], shape)
            line = jnp.take_along_axis(line, lanes, axis=1)
            value = line if value is None else jnp.where(item < sub, value, line)
        out_ref[r] = value.reshape(nx, nt, LANES)[:, :, :TMAX]


def kernel(
    dims, lx_ref, lt_ref, out_ref, raw, first, block, send, recv, lines, edge, middle, step_t, trans, part,
    gath, in_sem, send_sem, recv_sem, send2_sem, recv2_sem, entered,
):
    gx, gy, ta, nx, nt, ns, sub = dims
    groups = gx * ta
    total_t = ta * nt
    mx, my, mt = lax.axis_index("gx"), lax.axis_index("gy"), lax.axis_index("ta")
    me = mt * gx + mx
    sites = nx * nt
    comps = 12
    short = 10

    offsets = [(a, b, c) for c in range(ta) for b in range(gy) for a in range(gx)]
    offsets = [o for o in reversed(offsets) if o != (0, 0, 0)]
    plane = [o for o in offsets if o[1] == 0]
    peers = [o for o in offsets if o[0] == 0 and o[2] == 0]

    def target(offset):
        a, b, c = offset
        return {
            "gx": lax.rem(mx + a, gx),
            "gy": lax.rem(my + b, gy),
            "ta": lax.rem(mt + c, ta),
        }

    barrier = pltpu.get_barrier_semaphore()
    for offset in plane + peers:
        pl.semaphore_signal(barrier, inc=1, device_id=target(offset), device_id_type=MESH)

    for f, ref in enumerate((lt_ref, lx_ref)):
        for c in range(2):
            pltpu.make_async_copy(
                ref.at[c, pl.ds(0, 6 * sites)],
                raw.at[f, pl.ds(c * 6 * sites, 6 * sites)],
                in_sem.at[f],
            ).start()

    with scope("p_load"):
        pltpu.make_async_copy(raw.at[0], raw.at[0], in_sem.at[0]).wait()
    with scope("p_local"):
        t_local = lax.broadcasted_iota(jnp.int32, (sites, LANES), 0) % nt
        x_local = lax.broadcasted_iota(jnp.int32, (sites, LANES), 0) // nt
        line = pair(raw[0].reshape(comps, sites, LANES))
        step = 1
        while step < nt:
            earlier = unit_where(t_local >= step, rolled(line, step, 1))
            line = product(earlier, full(line))
            step *= 2
        first[...] = flat(line).reshape(comps * sites, LANES)
        for k in range(2):
            for m in range(3):
                for xl in range(2):
                    block[k, pl.ds(short * ROWS + m * ROWS + xl * 4, 4), :] = first[
                        pl.ds(4 * m * sites + (2 * k + xl) * nt + nt - 1, 4, stride=sites), :
                    ]
            for tt in range(2):
                block[k, pl.ds(short * ROWS + 2 * comps + tt * comps, comps), :] = first[
                    pl.ds(2 * k + tt, comps, stride=sites), :
                ]
        gauge = unit_where(t_local >= 1, rolled(line, 1, 1))
        pltpu.make_async_copy(raw.at[1], raw.at[1], in_sem.at[1]).wait()
        link = full(pair(raw[1].reshape(comps, sites, LANES)))
        beyond = unit_where(x_local < nx - 1, rolled(full(gauge), sites - nt, 1))
        parts = shorten(product_dagger(product(gauge, link), beyond))
        for k in range(2):
            for c in range(short):
                block[k, pl.ds(c * ROWS, ROWS), :] = parts[c][k * ROWS : (k + 1) * ROWS]
            send[:, pl.ds(k * sub, sub), :] = block[k].T.reshape(groups, sub, LANES)

    with scope("p_bar"):
        pl.semaphore_wait(barrier, len(plane + peers))
    for offset in peers:
        pl.semaphore_signal(entered, inc=1, device_id=target(offset), device_id_type=MESH)

    for k, offset in enumerate(plane):
        where = target(offset)
        pltpu.make_async_remote_copy(
            src_ref=send.at[where["ta"] * gx + where["gx"]],
            dst_ref=recv.at[me],
            send_sem=send_sem,
            recv_sem=recv_sem.at[mt // 2],
            device_id=where,
            device_id_type=MESH,
        ).start()
    own = pltpu.make_async_copy(send.at[me], recv.at[me], recv_sem.at[mt // 2])
    own.start()

    def next_x(mat):
        return tuple(
            pltpu.roll(m.reshape(-1, LANES), LANES - sub, 1).reshape(m.shape) for m in mat
        )

    t_half = lax.broadcasted_iota(jnp.int32, (ROWS, LANES), 0) % nt
    x_lane = lax.broadcasted_iota(jnp.int32, (ROWS, LANES), 1) // sub % nx
    for order in range(2):
        half = lax.rem(mt // 2 + order, 2)
        landed = recv.at[pl.ds(half * 2 * gx, 2 * gx)]
        with scope(f"p_w{order}"):
            pltpu.make_async_copy(landed, landed, recv_sem.at[half]).wait()
        with scope(f"p_half{order}"):
            got = recv[pl.ds(half * 2 * gx, 2 * gx)].reshape(2, gx, 2, sub, LANES)
            got = jnp.stack([jnp.stack([got[0, a, k], got[1, a, k]]) for a in range(gx) for k in range(2)])
            got = got.reshape(LANES, LANES).T
            parts = swap(got[: short * ROWS].reshape(short, ROWS, LANES), sub)
            ends = swap(got[short * ROWS : short * ROWS + 2 * comps].reshape(3, ROWS, LANES), sub)
            for m in range(3):
                for td in range(2):
                    lines[pl.ds(4 * m * ROWS + half * 2 + td + 1, 4, stride=ROWS), :] = ends[m, td * 4 : td * 4 + 4]
            starts = got[short * ROWS + 2 * comps :]
            for td in range(2):
                near = pltpu.roll(starts, LANES - sub * (1 + td), 1)
                far = pltpu.roll(starts, LANES - sub * (3 + td), 1)
                edge[pl.ds(td * nt + 1, comps, stride=ROWS), :] = near[:comps]
                edge[pl.ds(td * nt + 2, comps, stride=ROWS), :] = near[comps:]
                edge[pl.ds(td * nt + 3, comps, stride=ROWS), :] = far[:comps]
            end = pair(edge[...].reshape(comps, ROWS, LANES))
            end = full(unit_where((t_half > 0) & (x_lane == nx - 1), end))
            middle[:, pl.ds(half * ROWS, ROWS), :] = flat(product_dagger(lengthen(parts), end))

    with scope("p_prefix"):
        row = lax.broadcasted_iota(jnp.int32, (ROWS, LANES), 0)
        hop = lines[...].reshape(comps, ROWS, LANES)
        hop = jnp.where(row == ta + 1, pltpu.roll(hop, ta, 1), hop)
        hop = unit_where((row > 0) & (row < ta + 2), pair(hop))
        step = 1
        while step < ta + 2:
            earlier = unit_where(row >= step, rolled(hop, step, 1))
            hop = product(earlier, full(hop))
            step *= 2
        hop = full(hop)
        step_t[0] = flat(hop).reshape(18 * ROWS, LANES)
        step_t[1] = flat(next_x(hop)).reshape(18 * ROWS, LANES)

    def spread_t(side, rows, v):
        out = []
        for c in range(18):
            if c % 9 >= 3 * rows:
                continue
            low, high = (
                jnp.broadcast_to(step_t[side, pl.ds(c * ROWS + 2 * v + td, 1), :], (ROWS, LANES))
                for td in range(2)
            )
            out.append(jnp.where(row < nt, low, high))
        return pair(jnp.stack(out))

    with scope("p_path"):
        for v in range(total_t // ROWS + 1):
            start = v * ROWS
            inner = pair(middle[:, pl.ds(start % total_t, ROWS), :])
            moved = product(spread_t(0, 2, v), full(product_dagger(inner, spread_t(1, 3, v))))
            path = moved
            moved = full(moved)
            trans[0, :, pl.ds(start, ROWS), :] = flat(moved)
            for r in range(1, RMAX):
                moved = next_x(moved)
                path = product(path, moved)
                trans[r, :, pl.ds(start, ROWS), :] = flat(full(path))

    lane = lax.broadcasted_iota(jnp.int32, (total_t, LANES), 1)
    row = lax.broadcasted_iota(jnp.int32, (total_t, LANES), 0)
    sums = []
    with scope("p_sums"):
        for r in range(RMAX):
            for u in range(1, TMAX + 1):
                halves = []
                for start in range(0, total_t, ROWS):
                    here = trans[r, :, pl.ds(start, ROWS), :]
                    there = trans[r, :, pl.ds(start + u, ROWS), :]
                    halves.append(jnp.sum(here * there, axis=0))
                sums.append(jnp.concatenate(halves, axis=0))

    def merge(items, width):
        if width == 0:
            return items[0]
        half = width
        low = [i for i in items[:half]]
        high = [i for i in items[half:]]
        first = merge(low, width // 2)
        first = first + pltpu.roll(first, LANES - width, 1)
        if not high:
            return first
        second = merge(high, width // 2)
        second = second + pltpu.roll(second, width, 1)
        return jnp.where((lane & width) == 0, first, second)

    def fold(items):
        return merge(items, sub // 2)

    block = LANES // gx
    with scope("p_fold"):
        for g in range(-(-len(sums) // sub)):
            value = fold(sums[g * sub : (g + 1) * sub])
            bit = 1
            while bit < gx:
                i_bit = (row & bit) != 0
                j_bit = ((lane // block) & bit) != 0
                up = pltpu.roll(pltpu.roll(value, total_t - bit, 0), block * bit, 1)
                down = pltpu.roll(pltpu.roll(value, bit, 0), LANES - block * bit, 1)
                value = jnp.where(i_bit == j_bit, value, jnp.where(j_bit, up, down))
                bit *= 2
            part[:, g, :] = value

    slot = my * groups + me
    pl.semaphore_wait(entered, len(peers))
    copies2 = []
    for k, offset in enumerate(offsets):
        where = target(offset)
        copies2.append(
            pltpu.make_async_remote_copy(
                src_ref=part.at[where["ta"] * gx + where["gx"]],
                dst_ref=gath.at[slot],
                send_sem=send2_sem,
                recv_sem=recv2_sem,
                device_id=where,
                device_id_type=MESH,
            )
        )
        copies2[-1].start()
    gath[pl.ds(slot, 1)] = part[pl.ds(me, 1)]
    with scope("p_wait2"):
        sent = send.at[pl.ds(0, len(plane))]
        pltpu.make_async_copy(sent, sent, send_sem).wait()
        landed = gath.at[pl.ds(0, len(offsets))]
        pltpu.make_async_copy(landed, landed, send2_sem).wait()
        pltpu.make_async_copy(landed, landed, recv2_sem).wait()
    spread(jnp.sum(gath[...], axis=0) / (3.0 * (ns * gy)), nx, nt, sub, out_ref)


def fast(dims, link_x, link_t):
    gx, gy, ta, nx, nt, ns, sub = dims
    groups = gx * ta
    total_t = ta * nt
    flat = (2, 9 * nx * nt, ns)
    rows = -(-RMAX * TMAX // sub)
    out = pl.pallas_call(
        functools.partial(kernel, dims),
        out_shape=pltpu.VMEM((RMAX, nx, nt, TMAX), jnp.float32),
        in_specs=[pl.BlockSpec(memory_space=pl.ANY)] * 2,
        out_specs=pl.BlockSpec(memory_space=pltpu.VMEM),
        scratch_shapes=[
            pltpu.VMEM((2, 12 * nx * nt, ns), jnp.float32),
            pltpu.VMEM((12 * nx * nt, ns), jnp.float32),
            pltpu.VMEM((2, LANES, ns), jnp.float32),
            pltpu.VMEM((groups, 2 * sub, LANES), jnp.float32),
            pltpu.VMEM((groups, 2 * sub, LANES), jnp.float32),
            pltpu.VMEM((12 * ROWS, LANES), jnp.float32),
            pltpu.VMEM((12 * ROWS, LANES), jnp.float32),
            pltpu.VMEM((12, total_t, LANES), jnp.float32),
            pltpu.VMEM((2, 18 * ROWS, LANES), jnp.float32),
            pltpu.VMEM((RMAX, 18, total_t + ROWS, LANES), jnp.float32),
            pltpu.VMEM((groups, rows, LANES), jnp.float32),
            pltpu.VMEM((gy * groups, rows, LANES), jnp.float32),
            pltpu.SemaphoreType.DMA((2,)),
            pltpu.SemaphoreType.DMA,
            pltpu.SemaphoreType.DMA((2,)),
            pltpu.SemaphoreType.DMA,
            pltpu.SemaphoreType.DMA,
            pltpu.SemaphoreType.REGULAR,
        ],
        compiler_params=pltpu.CompilerParams(collective_id=0, has_side_effects=True),
        name="wilson",
    )(link_x.reshape(flat), link_t.reshape(flat))
    return out.transpose(0, 3, 1, 2)


def times(left, right):
    def dot(a, b):
        return sum(a[:, j][:, None] * b[j][None] for j in range(3))

    real = dot(left[0], right[0]) - dot(left[1], right[1])
    imag = dot(left[0], right[1]) + dot(left[1], right[0])
    return jnp.stack([real, imag])


def general(dims, link_x, link_t):
    gx, gy, ta, nx, nt, ns, sub = dims

    def gather(field):
        field = lax.all_to_all(field, "gx", 5, 3, tiled=True)
        return lax.all_to_all(field, "ta", 5, 4, tiled=True)

    link_x, link_t = gather(link_x), gather(link_t)

    def grow_t(carry, _):
        line, factor = carry
        factor = jnp.roll(factor, -1, axis=4)
        return (times(line, factor), factor), line

    _, temporal = lax.scan(grow_t, (link_t, link_t), None, length=TMAX)

    def radius(carry, _):
        spatial, factor, carried = carry
        carried = jnp.roll(carried, -1, axis=4)

        def extent(shifted, pair):
            line, line_r = pair
            shifted = jnp.roll(shifted, -1, axis=4)
            return shifted, jnp.sum(times(spatial, line_r) * times(line, shifted), axis=(0, 1, 2, 5))

        _, sums = lax.scan(extent, spatial, (temporal, carried))
        factor = jnp.roll(factor, -1, axis=3)
        return (times(spatial, factor), factor, carried), sums

    _, loops = lax.scan(radius, (link_x, link_x, temporal), None, length=RMAX)
    loops = lax.psum(loops, ("gx", "gy", "ta"))
    loops = lax.dynamic_slice_in_dim(loops, lax.axis_index("gx") * nx, nx, axis=2)
    loops = lax.dynamic_slice_in_dim(loops, lax.axis_index("ta") * nt, nt, axis=3)
    return loops / (3.0 * (ns * gy))


def local(link_x, link_t):
    gx, gy, ta = (lax.axis_size(a) for a in ("gx", "gy", "ta"))
    nx, nt, ns = link_x.shape[3:]
    sub = ns // (gx * ta)
    dims = (gx, gy, ta, nx, nt, ns, sub)
    fits = (
        ns == LANES
        and sub == ROWS
        and gx == nx == nt == ta == 4
    )
    return (fast if fits else general)(dims, link_x, link_t)


def solution(mesh):
    spec = P(None, None, None, "gx", "ta", "gy")
    return jax.shard_map(
        local,
        mesh=mesh,
        in_specs=(spec, spec),
        out_specs=P(None, None, "gx", "ta"),
        check_vma=False,
    )
```

```python
import contextlib
import functools

import jax
import jax.numpy as jnp
from jax import lax
from jax.experimental import pallas as pl
from jax.experimental.pallas import tpu as pltpu
from jax.sharding import PartitionSpec as P

RMAX = 6
TMAX = 6
LANES = 128
ROWS = 8
MESH = pl.DeviceIdType.MESH
scope = lambda name: contextlib.nullcontext()


def product(left, right):
    (ar, ai), (br, bi) = left, right
    real = imag = None
    for j in range(3):
        a_re, a_im = ar[:, j][:, None], ai[:, j][:, None]
        b_re, b_im = br[j][None], bi[j][None]
        re = a_re * b_re - a_im * b_im
        im = a_re * b_im + a_im * b_re
        real = re if real is None else real + re
        imag = im if imag is None else imag + im
    return real, imag


def product_dagger(left, right):
    (ar, ai), (br, bi) = left, right
    real = imag = None
    for j in range(3):
        a_re, a_im = ar[:, j][:, None], ai[:, j][:, None]
        b_re, b_im = br[:, j][None], bi[:, j][None]
        re = a_re * b_re + a_im * b_im
        im = a_im * b_re - a_re * b_im
        real = re if real is None else real + re
        imag = im if imag is None else imag + im
    return real, imag


def third(two):
    (ar, br), (ai, bi) = ((m[0], m[1]) for m in two)
    real, imag = [], []
    for k in range(3):
        p, q = (k + 1) % 3, (k + 2) % 3
        real.append(ar[p] * br[q] - ai[p] * bi[q] - ar[q] * br[p] + ai[q] * bi[p])
        imag.append(ar[q] * bi[p] + ai[q] * br[p] - ar[p] * bi[q] - ai[p] * br[q])
    return jnp.stack(real), jnp.stack(imag)


def full(two):
    return tuple(jnp.concatenate([m, t[None]], axis=0) for m, t in zip(two, third(two)))


def unit_where(mask, mat):
    rows = mat[0].shape[0]
    real = [
        jnp.stack([jnp.where(mask, mat[0][i, k], 1.0 if i == k else 0.0) for k in range(3)])
        for i in range(rows)
    ]
    return jnp.stack(real), jnp.where(mask, mat[1], 0.0)


def rolled(mat, shift, axis):
    return tuple(
        pltpu.roll(m.reshape(-1, *m.shape[2:]), shift, axis).reshape(m.shape) for m in mat
    )


def pivot(mat):
    size = [jnp.maximum(jnp.abs(mat[0][0, k]), jnp.abs(mat[1][0, k])) for k in range(3)]
    first = (size[0] >= size[1]) & (size[0] >= size[2])
    return first, size[1] >= size[2]


def choose(masks, a, b, c):
    return jnp.where(masks[0], a, jnp.where(masks[1], b, c))


def shorten(mat):
    masks = pivot(mat)
    parts = [m[0, k] for m in mat for k in range(3)]
    for m in mat:
        b = m[1]
        parts.append(choose(masks, b[1], b[2], b[0]))
        parts.append(choose(masks, b[2], b[0], b[1]))
    return parts


def lengthen(parts):
    ar, ai = parts[0:3], parts[3:6]
    (pr, qr), (pi, qi) = parts[6:8], parts[8:10]
    masks = pivot((parts[None, 0:3], parts[None, 3:6]))
    cr, ci = (choose(masks, a[0], a[1], a[2]) for a in (ar, ai))
    dr, di = (choose(masks, a[1], a[2], a[0]) for a in (ar, ai))
    er, ei = (choose(masks, a[2], a[0], a[1]) for a in (ar, ai))
    wr = dr * pr + di * pi + er * qr + ei * qi
    wi = dr * pi - di * pr + er * qi - ei * qr
    scale = -1.0 / (cr * cr + ci * ci)
    kr, ki = (wr * cr - wi * ci) * scale, (wr * ci + wi * cr) * scale
    second = []
    for k, p, q in ((kr, pr, qr), (ki, pi, qi)):
        second.append(jnp.stack([choose(masks, k, q, p), choose(masks, p, k, q), choose(masks, q, p, k)]))
    return jnp.stack([ar, second[0]]), jnp.stack([ai, second[1]])


def pair(block):
    half = block.reshape(2, -1, *block.shape[1:])
    return tuple(m.reshape(-1, 3, *block.shape[1:]) for m in half)


def flat(mat):
    return jnp.concatenate([m.reshape(-1, *m.shape[2:]) for m in mat], axis=0)


def join(early, late, sub):
    row = lax.broadcasted_iota(jnp.int32, early.shape, 1) // (ROWS // 2)
    lane = lax.broadcasted_iota(jnp.int32, early.shape, 2) // sub % 2
    early_turned, late_turned = (pltpu.roll(b, ROWS // 2, 1) for b in (early, late))
    even = jnp.where(row == 0, early, late_turned)
    odd = jnp.where(row == 0, early_turned, late)
    return jnp.where(lane == 0, even, odd)


def spread(total, nx, nt, sub, out_ref):
    shape = (nx * nt, LANES)
    corner = lax.broadcasted_iota(jnp.int32, shape, 0)
    column = lax.broadcasted_iota(jnp.int32, shape, 1)
    base = (corner // nt) * (sub * nt) + corner % nt
    for r in range(RMAX):
        first = r * TMAX // sub
        item = jnp.minimum(column + (r * TMAX - first * sub), 2 * sub - 1)
        lanes = base + item % sub * nt
        value = None
        for g in range(first, (r * TMAX + TMAX - 1) // sub + 1):
            line = jnp.broadcast_to(total[g : g + 1], shape)
            line = jnp.take_along_axis(line, lanes, axis=1)
            value = line if value is None else jnp.where(item < sub, value, line)
        out_ref[r] = value.reshape(nx, nt, LANES)[:, :, :TMAX]


def kernel(
    dims, lx_ref, lt_ref, out_ref, raw, first, block, send, recv, lines, edge, middle, step_t, trans, part,
    gath, in_sem, send_sem, recv_sem, send2_sem, recv2_sem, entered,
):
    gx, gy, ta, nx, nt, ns, sub = dims
    groups = gx * ta
    total_t = ta * nt
    mx, my, mt = lax.axis_index("gx"), lax.axis_index("gy"), lax.axis_index("ta")
    me = mt * gx + mx
    sites = nx * nt
    comps = 12
    short = 10

    offsets = [(a, b, c) for c in range(ta) for b in range(gy) for a in range(gx)]
    offsets = [o for o in reversed(offsets) if o != (0, 0, 0)]
    plane = [o for o in offsets if o[1] == 0]
    peers = [o for o in offsets if o[0] == 0 and o[2] == 0]

    def target(offset):
        a, b, c = offset
        return {
            "gx": lax.rem(mx + a, gx),
            "gy": lax.rem(my + b, gy),
            "ta": lax.rem(mt + c, ta),
        }

    barrier = pltpu.get_barrier_semaphore()
    for offset in plane + peers:
        pl.semaphore_signal(barrier, inc=1, device_id=target(offset), device_id_type=MESH)

    for f, ref in enumerate((lt_ref, lx_ref)):
        for c in range(2):
            pltpu.make_async_copy(
                ref.at[c, pl.ds(0, 6 * sites)],
                raw.at[f, pl.ds(c * 6 * sites, 6 * sites)],
                in_sem.at[f],
            ).start()

    with scope("p_load"):
        pltpu.make_async_copy(raw.at[0], raw.at[0], in_sem.at[0]).wait()
    with scope("p_local"):
        t_local = lax.broadcasted_iota(jnp.int32, (sites, LANES), 0) % nt
        x_local = lax.broadcasted_iota(jnp.int32, (sites, LANES), 0) // nt
        line = pair(raw[0].reshape(comps, sites, LANES))
        step = 1
        while step < nt:
            earlier = unit_where(t_local >= step, rolled(line, step, 1))
            line = product(earlier, full(line))
            step *= 2
        first[...] = flat(line).reshape(comps * sites, LANES)
        for k in range(2):
            for m in range(3):
                for xl in range(2):
                    block[k, pl.ds(short * ROWS + m * ROWS + xl * 4, 4), :] = first[
                        pl.ds(4 * m * sites + (2 * k + xl) * nt + nt - 1, 4, stride=sites), :
                    ]
            for tt in range(2):
                block[k, pl.ds(short * ROWS + 2 * comps + tt * comps, comps), :] = first[
                    pl.ds(2 * k + tt, comps, stride=sites), :
                ]
        gauge = unit_where(t_local >= 1, rolled(line, 1, 1))
        pltpu.make_async_copy(raw.at[1], raw.at[1], in_sem.at[1]).wait()
        link = full(pair(raw[1].reshape(comps, sites, LANES)))
        beyond = unit_where(x_local < nx - 1, rolled(full(gauge), sites - nt, 1))
        parts = shorten(product_dagger(product(gauge, link), beyond))
        for k in range(2):
            for c in range(short):
                block[k, pl.ds(c * ROWS, ROWS), :] = parts[c][k * ROWS : (k + 1) * ROWS]
            send[:, pl.ds(k * sub, sub), :] = block[k].T.reshape(groups, sub, LANES)

    with scope("p_bar"):
        pl.semaphore_wait(barrier, len(plane + peers))
    for offset in peers:
        pl.semaphore_signal(entered, inc=1, device_id=target(offset), device_id_type=MESH)

    for k, offset in enumerate(plane):
        where = target(offset)
        pltpu.make_async_remote_copy(
            src_ref=send.at[where["ta"] * gx + where["gx"]],
            dst_ref=recv.at[me],
            send_sem=send_sem,
            recv_sem=recv_sem.at[mt // 2],
            device_id=where,
            device_id_type=MESH,
        ).start()
    own = pltpu.make_async_copy(send.at[me], recv.at[me], recv_sem.at[mt // 2])
    own.start()

    def next_x(mat):
        return tuple(
            pltpu.roll(m.reshape(-1, LANES), LANES - sub, 1).reshape(m.shape) for m in mat
        )

    t_half = lax.broadcasted_iota(jnp.int32, (ROWS, LANES), 0) % nt
    x_lane = lax.broadcasted_iota(jnp.int32, (ROWS, LANES), 1) // sub % nx
    for order in range(2):
        half = lax.rem(mt // 2 + order, 2)
        landed = recv.at[pl.ds(half * 2 * gx, 2 * gx)]
        with scope(f"p_w{order}"):
            pltpu.make_async_copy(landed, landed, recv_sem.at[half]).wait()
        with scope(f"p_half{order}"):
            got = recv[pl.ds(half * 2 * gx, 2 * gx)].reshape(2, gx * 2, sub, LANES)
            got = [jnp.stack([got[td], got[td]], axis=1).reshape(LANES, LANES).T for td in range(2)]
            cuts = short * ROWS, short * ROWS + 2 * comps
            parts = join(*(g[: cuts[0]].reshape(short, ROWS, LANES) for g in got), sub)
            ends = join(*(g[cuts[0] : cuts[1]].reshape(3, ROWS, LANES) for g in got), sub)
            for m in range(3):
                for td in range(2):
                    lines[pl.ds(4 * m * ROWS + half * 2 + td + 1, 4, stride=ROWS), :] = ends[m, td * 4 : td * 4 + 4]
            for td in range(2):
                near = pltpu.roll(got[td][cuts[1] :], LANES - sub, 1)
                far = pltpu.roll(got[td][cuts[1] : cuts[1] + 2 * ROWS], LANES - 3 * sub, 1)
                edge[pl.ds(td * nt + 1, comps, stride=ROWS), :] = near[:comps]
                edge[pl.ds(td * nt + 2, comps, stride=ROWS), :] = near[comps:]
                edge[pl.ds(td * nt + 3, comps, stride=ROWS), :] = far[:comps]
            end = pair(edge[...].reshape(comps, ROWS, LANES))
            end = full(unit_where((t_half > 0) & (x_lane == nx - 1), end))
            middle[:, pl.ds(half * ROWS, ROWS), :] = flat(product_dagger(lengthen(parts), end))

    with scope("p_prefix"):
        row = lax.broadcasted_iota(jnp.int32, (ROWS, LANES), 0)
        hop = lines[...].reshape(comps, ROWS, LANES)
        hop = jnp.where(row == ta + 1, pltpu.roll(hop, ta, 1), hop)
        hop = unit_where((row > 0) & (row < ta + 2), pair(hop))
        step = 1
        while step < ta + 2:
            earlier = unit_where(row >= step, rolled(hop, step, 1))
            hop = product(earlier, full(hop))
            step *= 2
        hop = full(hop)
        step_t[0] = flat(hop).reshape(18 * ROWS, LANES)
        step_t[1] = flat(next_x(hop)).reshape(18 * ROWS, LANES)

    def spread_t(side, rows, v):
        out = []
        for c in range(18):
            if c % 9 >= 3 * rows:
                continue
            low, high = (
                jnp.broadcast_to(step_t[side, pl.ds(c * ROWS + 2 * v + td, 1), :], (ROWS, LANES))
                for td in range(2)
            )
            out.append(jnp.where(row < nt, low, high))
        return pair(jnp.stack(out))

    row_t = row // nt
    lane = lax.broadcasted_iota(jnp.int32, (ROWS, LANES), 1)
    block_x = lane // (LANES // nx)
    own_time = row % nt * (LANES // nx) + lane % (LANES // nx)

    def emit(items, g, held):
        stack = []
        for td in range(ta):
            for a, b in zip(items[::2], items[1::2]):
                a, b = a[td // 2], b[td // 2]
                if td % 2:
                    stack.append(jnp.where(row_t == 0, pltpu.roll(a, nt, 0), b))
                else:
                    stack.append(jnp.where(row_t == 0, a, pltpu.roll(b, nt, 0)))
            stack += [jnp.zeros((ROWS, LANES), jnp.float32)] * ((sub - len(items)) // 2)
        turned = jnp.concatenate(stack, axis=0).T.reshape(gx * nx, sub, LANES)
        for step in (4, 2, 1):
            turned = turned + pltpu.roll(turned, step, 1)
        if g % 2 == 0 and g < rows - 1:
            return turned
        low = turned if held is None else held
        for j in range(gx):
            value = None
            for x in range(nx):
                both = jnp.where(row_t == 0, low[j * nx + x], turned[j * nx + x])
                both = jnp.take_along_axis(both, own_time, axis=1)
                value = both if value is None else jnp.where(block_x == x, both, value)
            for k in range(1 if held is None else 2):
                part[pl.ds(j * ROWS + g // 2 * 2 + k, ta, stride=gx * ROWS), :] = value[k * nt : k * nt + ta]
        return None

    rows = -(-RMAX * TMAX // sub)
    with scope("p_path"):
        for v in range(total_t // ROWS + 1):
            start = v * ROWS
            inner = pair(middle[:, pl.ds(start % total_t, ROWS), :])
            moved = product(spread_t(0, 2, v), full(product_dagger(inner, spread_t(1, 3, v))))
            trans[0, :, pl.ds(start, ROWS), :] = flat(full(moved))
    with scope("p_sums"):
        items, g, held = [], 0, None
        for r in range(RMAX):
            for v in range(total_t // ROWS + 1) if r else ():
                here = pl.ds(v * ROWS, ROWS)
                moved = pair(pltpu.roll(trans[0, :, here, :].reshape(-1, LANES), LANES - r * sub, 1).reshape(18, ROWS, LANES))
                path = pair(trans[r - 1, :, here, :])
                path = product((path[0][:2], path[1][:2]), moved)
                trans[r, :, here, :] = flat(full(path))
            for u in range(1, TMAX + 1):
                items.append(
                    [
                        jnp.sum(trans[r, :, pl.ds(start, ROWS), :] * trans[r, :, pl.ds(start + u, ROWS), :], axis=0)
                        for start in range(0, total_t, ROWS)
                    ]
                )
                if len(items) == sub or (r, u) == (RMAX - 1, TMAX):
                    held = emit(items, g, held)
                    items, g = [], g + 1

    slot = my * groups + me
    pl.semaphore_wait(entered, len(peers))
    copies2 = []
    for k, offset in enumerate(offsets):
        where = target(offset)
        copies2.append(
            pltpu.make_async_remote_copy(
                src_ref=part.at[pl.ds((where["ta"] * gx + where["gx"]) * ROWS, rows)],
                dst_ref=gath.at[slot],
                send_sem=send2_sem,
                recv_sem=recv2_sem,
                device_id=where,
                device_id_type=MESH,
            )
        )
        copies2[-1].start()
    gath[slot] = part[pl.ds(me * ROWS, rows), :]
    with scope("p_wait2"):
        sent = send.at[pl.ds(0, len(plane))]
        pltpu.make_async_copy(sent, sent, send_sem).wait()
        landed = gath.at[pl.ds(0, len(offsets))]
        pltpu.make_async_copy(landed, landed, send2_sem).wait()
        pltpu.make_async_copy(landed, landed, recv2_sem).wait()
    spread(jnp.sum(gath[...], axis=0) / (3.0 * (ns * gy)), nx, nt, sub, out_ref)


def fast(dims, link_x, link_t):
    gx, gy, ta, nx, nt, ns, sub = dims
    groups = gx * ta
    total_t = ta * nt
    flat = (2, 9 * nx * nt, ns)
    rows = -(-RMAX * TMAX // sub)
    out = pl.pallas_call(
        functools.partial(kernel, dims),
        out_shape=pltpu.VMEM((RMAX, nx, nt, TMAX), jnp.float32),
        in_specs=[pl.BlockSpec(memory_space=pl.ANY)] * 2,
        out_specs=pl.BlockSpec(memory_space=pltpu.VMEM),
        scratch_shapes=[
            pltpu.VMEM((2, 12 * nx * nt, ns), jnp.float32),
            pltpu.VMEM((12 * nx * nt, ns), jnp.float32),
            pltpu.VMEM((2, LANES, ns), jnp.float32),
            pltpu.VMEM((groups, 2 * sub, LANES), jnp.float32),
            pltpu.VMEM((groups, 2 * sub, LANES), jnp.float32),
            pltpu.VMEM((12 * ROWS, LANES), jnp.float32),
            pltpu.VMEM((12 * ROWS, LANES), jnp.float32),
            pltpu.VMEM((12, total_t, LANES), jnp.float32),
            pltpu.VMEM((2, 18 * ROWS, LANES), jnp.float32),
            pltpu.VMEM((RMAX, 18, total_t + ROWS, LANES), jnp.float32),
            pltpu.VMEM((groups * ROWS, LANES), jnp.float32),
            pltpu.VMEM((gy * groups, rows, LANES), jnp.float32),
            pltpu.SemaphoreType.DMA((2,)),
            pltpu.SemaphoreType.DMA,
            pltpu.SemaphoreType.DMA((2,)),
            pltpu.SemaphoreType.DMA,
            pltpu.SemaphoreType.DMA,
            pltpu.SemaphoreType.REGULAR,
        ],
        compiler_params=pltpu.CompilerParams(collective_id=0, has_side_effects=True),
        name="wilson",
    )(link_x.reshape(flat), link_t.reshape(flat))
    return out.transpose(0, 3, 1, 2)


def times(left, right):
    def dot(a, b):
        return sum(a[:, j][:, None] * b[j][None] for j in range(3))

    real = dot(left[0], right[0]) - dot(left[1], right[1])
    imag = dot(left[0], right[1]) + dot(left[1], right[0])
    return jnp.stack([real, imag])


def general(dims, link_x, link_t):
    gx, gy, ta, nx, nt, ns, sub = dims

    def gather(field):
        field = lax.all_to_all(field, "gx", 5, 3, tiled=True)
        return lax.all_to_all(field, "ta", 5, 4, tiled=True)

    link_x, link_t = gather(link_x), gather(link_t)

    def grow_t(carry, _):
        line, factor = carry
        factor = jnp.roll(factor, -1, axis=4)
        return (times(line, factor), factor), line

    _, temporal = lax.scan(grow_t, (link_t, link_t), None, length=TMAX)

    def radius(carry, _):
        spatial, factor, carried = carry
        carried = jnp.roll(carried, -1, axis=4)

        def extent(shifted, pair):
            line, line_r = pair
            shifted = jnp.roll(shifted, -1, axis=4)
            return shifted, jnp.sum(times(spatial, line_r) * times(line, shifted), axis=(0, 1, 2, 5))

        _, sums = lax.scan(extent, spatial, (temporal, carried))
        factor = jnp.roll(factor, -1, axis=3)
        return (times(spatial, factor), factor, carried), sums

    _, loops = lax.scan(radius, (link_x, link_x, temporal), None, length=RMAX)
    loops = lax.psum(loops, ("gx", "gy", "ta"))
    loops = lax.dynamic_slice_in_dim(loops, lax.axis_index("gx") * nx, nx, axis=2)
    loops = lax.dynamic_slice_in_dim(loops, lax.axis_index("ta") * nt, nt, axis=3)
    return loops / (3.0 * (ns * gy))


def local(link_x, link_t):
    gx, gy, ta = (lax.axis_size(a) for a in ("gx", "gy", "ta"))
    nx, nt, ns = link_x.shape[3:]
    sub = ns // (gx * ta)
    dims = (gx, gy, ta, nx, nt, ns, sub)
    fits = (
        ns == LANES
        and sub == ROWS
        and gx == nx == nt == ta == 4
    )
    return (fast if fits else general)(dims, link_x, link_t)


def solution(mesh):
    spec = P(None, None, None, "gx", "ta", "gy")
    return jax.shard_map(
        local,
        mesh=mesh,
        in_specs=(spec, spec),
        out_specs=P(None, None, "gx", "ta"),
        check_vma=False,
    )
```

```python
import contextlib
import functools

import jax
import jax.numpy as jnp
from jax import lax
from jax.experimental import pallas as pl
from jax.experimental.pallas import tpu as pltpu
from jax.sharding import PartitionSpec as P

RMAX = 6
TMAX = 6
LANES = 128
ROWS = 8
MESH = pl.DeviceIdType.MESH
scope = lambda name: contextlib.nullcontext()


def product(left, right):
    (ar, ai), (br, bi) = left, right
    real = imag = None
    for j in range(3):
        a_re, a_im = ar[:, j][:, None], ai[:, j][:, None]
        b_re, b_im = br[j][None], bi[j][None]
        re = a_re * b_re - a_im * b_im
        im = a_re * b_im + a_im * b_re
        real = re if real is None else real + re
        imag = im if imag is None else imag + im
    return real, imag


def product_dagger(left, right):
    (ar, ai), (br, bi) = left, right
    real = imag = None
    for j in range(3):
        a_re, a_im = ar[:, j][:, None], ai[:, j][:, None]
        b_re, b_im = br[:, j][None], bi[:, j][None]
        re = a_re * b_re + a_im * b_im
        im = a_im * b_re - a_re * b_im
        real = re if real is None else real + re
        imag = im if imag is None else imag + im
    return real, imag


def third(two):
    (ar, br), (ai, bi) = ((m[0], m[1]) for m in two)
    real, imag = [], []
    for k in range(3):
        p, q = (k + 1) % 3, (k + 2) % 3
        real.append(ar[p] * br[q] - ai[p] * bi[q] - ar[q] * br[p] + ai[q] * bi[p])
        imag.append(ar[q] * bi[p] + ai[q] * br[p] - ar[p] * bi[q] - ai[p] * br[q])
    return jnp.stack(real), jnp.stack(imag)


def full(two):
    return tuple(jnp.concatenate([m, t[None]], axis=0) for m, t in zip(two, third(two)))


def unit_where(mask, mat):
    rows = mat[0].shape[0]
    real = [
        jnp.stack([jnp.where(mask, mat[0][i, k], 1.0 if i == k else 0.0) for k in range(3)])
        for i in range(rows)
    ]
    return jnp.stack(real), jnp.where(mask, mat[1], 0.0)


def rolled(mat, shift, axis):
    return tuple(
        pltpu.roll(m.reshape(-1, *m.shape[2:]), shift, axis).reshape(m.shape) for m in mat
    )


def pivot(mat):
    size = [jnp.maximum(jnp.abs(mat[0][0, k]), jnp.abs(mat[1][0, k])) for k in range(3)]
    first = (size[0] >= size[1]) & (size[0] >= size[2])
    return first, size[1] >= size[2]


def choose(masks, a, b, c):
    return jnp.where(masks[0], a, jnp.where(masks[1], b, c))


def shorten(mat):
    masks = pivot(mat)
    parts = [m[0, k] for m in mat for k in range(3)]
    for m in mat:
        b = m[1]
        parts.append(choose(masks, b[1], b[2], b[0]))
        parts.append(choose(masks, b[2], b[0], b[1]))
    return parts


def lengthen(parts):
    ar, ai = parts[0:3], parts[3:6]
    (pr, qr), (pi, qi) = parts[6:8], parts[8:10]
    masks = pivot((parts[None, 0:3], parts[None, 3:6]))
    cr, ci = (choose(masks, a[0], a[1], a[2]) for a in (ar, ai))
    dr, di = (choose(masks, a[1], a[2], a[0]) for a in (ar, ai))
    er, ei = (choose(masks, a[2], a[0], a[1]) for a in (ar, ai))
    wr = dr * pr + di * pi + er * qr + ei * qi
    wi = dr * pi - di * pr + er * qi - ei * qr
    scale = -1.0 / (cr * cr + ci * ci)
    kr, ki = (wr * cr - wi * ci) * scale, (wr * ci + wi * cr) * scale
    second = []
    for k, p, q in ((kr, pr, qr), (ki, pi, qi)):
        second.append(jnp.stack([choose(masks, k, q, p), choose(masks, p, k, q), choose(masks, q, p, k)]))
    return jnp.stack([ar, second[0]]), jnp.stack([ai, second[1]])


def pair(block):
    half = block.reshape(2, -1, *block.shape[1:])
    return tuple(m.reshape(-1, 3, *block.shape[1:]) for m in half)


def flat(mat):
    return jnp.concatenate([m.reshape(-1, *m.shape[2:]) for m in mat], axis=0)


def join(early, late, sub):
    row = lax.broadcasted_iota(jnp.int32, early.shape, 1) // (ROWS // 2)
    lane = lax.broadcasted_iota(jnp.int32, early.shape, 2) // sub % 2
    early_turned, late_turned = (pltpu.roll(b, ROWS // 2, 1) for b in (early, late))
    even = jnp.where(row == 0, early, late_turned)
    odd = jnp.where(row == 0, early_turned, late)
    return jnp.where(lane == 0, even, odd)


def spread(total, nx, nt, sub, out_ref):
    shape = (nx * nt, LANES)
    corner = lax.broadcasted_iota(jnp.int32, shape, 0)
    column = lax.broadcasted_iota(jnp.int32, shape, 1)
    base = (corner // nt) * (sub * nt) + corner % nt
    for r in range(RMAX):
        first = r * TMAX // sub
        item = jnp.minimum(column + (r * TMAX - first * sub), 2 * sub - 1)
        lanes = base + item % sub * nt
        value = None
        for g in range(first, (r * TMAX + TMAX - 1) // sub + 1):
            line = jnp.broadcast_to(total[g : g + 1], shape)
            line = jnp.take_along_axis(line, lanes, axis=1)
            value = line if value is None else jnp.where(item < sub, value, line)
        out_ref[r] = value.reshape(nx, nt, LANES)[:, :, :TMAX]


def kernel(
    dims, lx_ref, lt_ref, out_ref, raw, first, block, send, recv, lines, edge, middle, step_t, trans, part,
    gath, in_sem, send_sem, recv_sem, send2_sem, recv2_sem, entered,
):
    gx, gy, ta, nx, nt, ns, sub = dims
    groups = gx * ta
    total_t = ta * nt
    mx, my, mt = lax.axis_index("gx"), lax.axis_index("gy"), lax.axis_index("ta")
    me = mt * gx + mx
    sites = nx * nt
    comps = 12
    short = 10

    steps = [(a, b, c, d) for a in range(2) for b in range(2) for c in range(gy) for d in range(ta)]
    steps = [o for o in steps if any(o)]
    plane = [o for o in steps if o[2] == 0]
    plane.sort(key=lambda o: (-o[3], -o[0], o[1]))
    steps.sort(key=lambda o: (-o[2], -min(o[3], ta - o[3]) - o[0], o[1], o[3]))
    peers = [o for o in steps if o[0] == o[1] == o[3] == 0]

    def target(step):
        a, b, c, d = step
        return {
            "gx": lax.rem(mx // 2 + a, 2) * 2 + lax.rem(mx + b, 2),
            "gy": lax.rem(my + c, gy),
            "ta": lax.rem(mt + d, ta),
        }

    barrier = pltpu.get_barrier_semaphore()
    for step in plane + peers:
        pl.semaphore_signal(barrier, inc=1, device_id=target(step), device_id_type=MESH)

    for f, ref in enumerate((lt_ref, lx_ref)):
        for c in range(2):
            pltpu.make_async_copy(
                ref.at[c, pl.ds(0, 6 * sites)],
                raw.at[f, pl.ds(c * 6 * sites, 6 * sites)],
                in_sem.at[f],
            ).start()

    with scope("p_load"):
        pltpu.make_async_copy(raw.at[0], raw.at[0], in_sem.at[0]).wait()
    with scope("p_local"):
        t_local = lax.broadcasted_iota(jnp.int32, (sites, LANES), 0) % nt
        x_local = lax.broadcasted_iota(jnp.int32, (sites, LANES), 0) // nt
        line = pair(raw[0].reshape(comps, sites, LANES))
        step = 1
        while step < nt:
            earlier = unit_where(t_local >= step, rolled(line, step, 1))
            line = product(earlier, full(line))
            step *= 2
        first[...] = flat(line).reshape(comps * sites, LANES)
        for k in range(2):
            for m in range(3):
                for xl in range(2):
                    block[k, pl.ds(short * ROWS + m * ROWS + xl * 4, 4), :] = first[
                        pl.ds(4 * m * sites + (2 * k + xl) * nt + nt - 1, 4, stride=sites), :
                    ]
            for tt in range(2):
                block[k, pl.ds(short * ROWS + 2 * comps + tt * comps, comps), :] = first[
                    pl.ds(2 * k + tt, comps, stride=sites), :
                ]
        gauge = unit_where(t_local >= 1, rolled(line, 1, 1))
        pltpu.make_async_copy(raw.at[1], raw.at[1], in_sem.at[1]).wait()
        link = full(pair(raw[1].reshape(comps, sites, LANES)))
        beyond = unit_where(x_local < nx - 1, rolled(full(gauge), sites - nt, 1))
        parts = shorten(product_dagger(product(gauge, link), beyond))
        for k in range(2):
            for c in range(short):
                block[k, pl.ds(c * ROWS, ROWS), :] = parts[c][k * ROWS : (k + 1) * ROWS]
            send[:, pl.ds(k * sub, sub), :] = block[k].T.reshape(groups, sub, LANES)

    with scope("p_bar"):
        pl.semaphore_wait(barrier, len(plane + peers))
    for step in peers:
        pl.semaphore_signal(entered, inc=1, device_id=target(step), device_id_type=MESH)

    for step in plane:
        where = target(step)
        pltpu.make_async_remote_copy(
            src_ref=send.at[where["ta"] * gx + where["gx"]],
            dst_ref=recv.at[me],
            send_sem=send_sem,
            recv_sem=recv_sem.at[mt // 2],
            device_id=where,
            device_id_type=MESH,
        ).start()
    own = pltpu.make_async_copy(send.at[me], recv.at[me], recv_sem.at[mt // 2])
    own.start()

    def next_x(mat):
        return tuple(
            pltpu.roll(m.reshape(-1, LANES), LANES - sub, 1).reshape(m.shape) for m in mat
        )

    t_half = lax.broadcasted_iota(jnp.int32, (ROWS, LANES), 0) % nt
    x_lane = lax.broadcasted_iota(jnp.int32, (ROWS, LANES), 1) // sub % nx
    for order in range(2):
        half = lax.rem(mt // 2 + order, 2)
        landed = recv.at[pl.ds(half * 2 * gx, 2 * gx)]
        with scope(f"p_w{order}"):
            pltpu.make_async_copy(landed, landed, recv_sem.at[half]).wait()
        with scope(f"p_half{order}"):
            got = recv[pl.ds(half * 2 * gx, 2 * gx)].reshape(2, gx * 2, sub, LANES)
            got = [jnp.stack([got[td], got[td]], axis=1).reshape(LANES, LANES).T for td in range(2)]
            cuts = short * ROWS, short * ROWS + 2 * comps
            parts = join(*(g[: cuts[0]].reshape(short, ROWS, LANES) for g in got), sub)
            ends = join(*(g[cuts[0] : cuts[1]].reshape(3, ROWS, LANES) for g in got), sub)
            for m in range(3):
                for td in range(2):
                    lines[pl.ds(4 * m * ROWS + half * 2 + td + 1, 4, stride=ROWS), :] = ends[m, td * 4 : td * 4 + 4]
            for td in range(2):
                near = pltpu.roll(got[td][cuts[1] :], LANES - sub, 1)
                far = pltpu.roll(got[td][cuts[1] : cuts[1] + 2 * ROWS], LANES - 3 * sub, 1)
                edge[pl.ds(td * nt + 1, comps, stride=ROWS), :] = near[:comps]
                edge[pl.ds(td * nt + 2, comps, stride=ROWS), :] = near[comps:]
                edge[pl.ds(td * nt + 3, comps, stride=ROWS), :] = far[:comps]
            end = pair(edge[...].reshape(comps, ROWS, LANES))
            end = full(unit_where((t_half > 0) & (x_lane == nx - 1), end))
            middle[:, pl.ds(half * ROWS, ROWS), :] = flat(product_dagger(lengthen(parts), end))

    with scope("p_prefix"):
        row = lax.broadcasted_iota(jnp.int32, (ROWS, LANES), 0)
        hop = lines[...].reshape(comps, ROWS, LANES)
        hop = jnp.where(row == ta + 1, pltpu.roll(hop, ta, 1), hop)
        hop = unit_where((row > 0) & (row < ta + 2), pair(hop))
        step = 1
        while step < ta + 2:
            earlier = unit_where(row >= step, rolled(hop, step, 1))
            hop = product(earlier, full(hop))
            step *= 2
        hop = full(hop)
        step_t[0] = flat(hop).reshape(18 * ROWS, LANES)
        step_t[1] = flat(next_x(hop)).reshape(18 * ROWS, LANES)

    def spread_t(side, rows, v):
        out = []
        for c in range(18):
            if c % 9 >= 3 * rows:
                continue
            low, high = (
                jnp.broadcast_to(step_t[side, pl.ds(c * ROWS + 2 * v + td, 1), :], (ROWS, LANES))
                for td in range(2)
            )
            out.append(jnp.where(row < nt, low, high))
        return pair(jnp.stack(out))

    row_t = row // nt
    lane = lax.broadcasted_iota(jnp.int32, (ROWS, LANES), 1)
    block_x = lane // (LANES // nx)
    own_time = row % nt * (LANES // nx) + lane % (LANES // nx)

    def emit(items, g, held):
        stack = []
        for td in range(ta):
            for a, b in zip(items[::2], items[1::2]):
                a, b = a[td // 2], b[td // 2]
                if td % 2:
                    stack.append(jnp.where(row_t == 0, pltpu.roll(a, nt, 0), b))
                else:
                    stack.append(jnp.where(row_t == 0, a, pltpu.roll(b, nt, 0)))
            stack += [jnp.zeros((ROWS, LANES), jnp.float32)] * ((sub - len(items)) // 2)
        turned = jnp.concatenate(stack, axis=0).T.reshape(gx * nx, sub, LANES)
        for step in (4, 2, 1):
            turned = turned + pltpu.roll(turned, step, 1)
        if g % 2 == 0 and g < rows - 1:
            return turned
        low = turned if held is None else held
        for j in range(gx):
            value = None
            for x in range(nx):
                both = jnp.where(row_t == 0, low[j * nx + x], turned[j * nx + x])
                both = jnp.take_along_axis(both, own_time, axis=1)
                value = both if value is None else jnp.where(block_x == x, both, value)
            for k in range(1 if held is None else 2):
                part[pl.ds(j * ROWS + g // 2 * 2 + k, ta, stride=gx * ROWS), :] = value[k * nt : k * nt + ta]
        return None

    rows = -(-RMAX * TMAX // sub)
    with scope("p_path"):
        for v in range(total_t // ROWS + 1):
            start = v * ROWS
            inner = pair(middle[:, pl.ds(start % total_t, ROWS), :])
            moved = product(spread_t(0, 2, v), full(product_dagger(inner, spread_t(1, 3, v))))
            trans[0, :, pl.ds(start, ROWS), :] = flat(full(moved))
    with scope("p_sums"):
        items, g, held = [], 0, None
        for r in range(RMAX):
            for v in range(total_t // ROWS + 1) if r else ():
                here = pl.ds(v * ROWS, ROWS)
                moved = pair(pltpu.roll(trans[0, :, here, :].reshape(-1, LANES), LANES - r * sub, 1).reshape(18, ROWS, LANES))
                path = pair(trans[r - 1, :, here, :])
                path = product((path[0][:2], path[1][:2]), moved)
                trans[r, :, here, :] = flat(full(path))
            for u in range(1, TMAX + 1):
                items.append(
                    [
                        jnp.sum(trans[r, :, pl.ds(start, ROWS), :] * trans[r, :, pl.ds(start + u, ROWS), :], axis=0)
                        for start in range(0, total_t, ROWS)
                    ]
                )
                if len(items) == sub or (r, u) == (RMAX - 1, TMAX):
                    held = emit(items, g, held)
                    items, g = [], g + 1

    slot = my * groups + me
    with scope("p_entered"):
        pl.semaphore_wait(entered, len(peers))
    with scope("p_send2"):
        for step in steps:
            where = target(step)
            pltpu.make_async_remote_copy(
                src_ref=part.at[pl.ds((where["ta"] * gx + where["gx"]) * ROWS, rows)],
                dst_ref=gath.at[slot],
                send_sem=send2_sem,
                recv_sem=recv2_sem,
                device_id=where,
                device_id_type=MESH,
            ).start()
    gath[slot] = part[pl.ds(me * ROWS, rows), :]
    with scope("p_wait2"):
        sent = send.at[pl.ds(0, len(plane))]
        pltpu.make_async_copy(sent, sent, send_sem).wait()
        landed = gath.at[pl.ds(0, len(steps))]
        pltpu.make_async_copy(landed, landed, send2_sem).wait()
        pltpu.make_async_copy(landed, landed, recv2_sem).wait()
    spread(jnp.sum(gath[...], axis=0) / (3.0 * (ns * gy)), nx, nt, sub, out_ref)


def fast(dims, link_x, link_t):
    gx, gy, ta, nx, nt, ns, sub = dims
    groups = gx * ta
    total_t = ta * nt
    flat = (2, 9 * nx * nt, ns)
    rows = -(-RMAX * TMAX // sub)
    out = pl.pallas_call(
        functools.partial(kernel, dims),
        out_shape=pltpu.VMEM((RMAX, nx, nt, TMAX), jnp.float32),
        in_specs=[pl.BlockSpec(memory_space=pl.ANY)] * 2,
        out_specs=pl.BlockSpec(memory_space=pltpu.VMEM),
        scratch_shapes=[
            pltpu.VMEM((2, 12 * nx * nt, ns), jnp.float32),
            pltpu.VMEM((12 * nx * nt, ns), jnp.float32),
            pltpu.VMEM((2, LANES, ns), jnp.float32),
            pltpu.VMEM((groups, 2 * sub, LANES), jnp.float32),
            pltpu.VMEM((groups, 2 * sub, LANES), jnp.float32),
            pltpu.VMEM((12 * ROWS, LANES), jnp.float32),
            pltpu.VMEM((12 * ROWS, LANES), jnp.float32),
            pltpu.VMEM((12, total_t, LANES), jnp.float32),
            pltpu.VMEM((2, 18 * ROWS, LANES), jnp.float32),
            pltpu.VMEM((RMAX, 18, total_t + ROWS, LANES), jnp.float32),
            pltpu.VMEM((groups * ROWS, LANES), jnp.float32),
            pltpu.VMEM((gy * groups, rows, LANES), jnp.float32),
            pltpu.SemaphoreType.DMA((2,)),
            pltpu.SemaphoreType.DMA,
            pltpu.SemaphoreType.DMA((2,)),
            pltpu.SemaphoreType.DMA,
            pltpu.SemaphoreType.DMA,
            pltpu.SemaphoreType.REGULAR,
        ],
        compiler_params=pltpu.CompilerParams(collective_id=0, has_side_effects=True),
        name="wilson",
    )(link_x.reshape(flat), link_t.reshape(flat))
    return out.transpose(0, 3, 1, 2)


def times(left, right):
    def dot(a, b):
        return sum(a[:, j][:, None] * b[j][None] for j in range(3))

    real = dot(left[0], right[0]) - dot(left[1], right[1])
    imag = dot(left[0], right[1]) + dot(left[1], right[0])
    return jnp.stack([real, imag])


def general(dims, link_x, link_t):
    gx, gy, ta, nx, nt, ns, sub = dims

    def gather(field):
        field = lax.all_to_all(field, "gx", 5, 3, tiled=True)
        return lax.all_to_all(field, "ta", 5, 4, tiled=True)

    link_x, link_t = gather(link_x), gather(link_t)

    def grow_t(carry, _):
        line, factor = carry
        factor = jnp.roll(factor, -1, axis=4)
        return (times(line, factor), factor), line

    _, temporal = lax.scan(grow_t, (link_t, link_t), None, length=TMAX)

    def radius(carry, _):
        spatial, factor, carried = carry
        carried = jnp.roll(carried, -1, axis=4)

        def extent(shifted, pair):
            line, line_r = pair
            shifted = jnp.roll(shifted, -1, axis=4)
            return shifted, jnp.sum(times(spatial, line_r) * times(line, shifted), axis=(0, 1, 2, 5))

        _, sums = lax.scan(extent, spatial, (temporal, carried))
        factor = jnp.roll(factor, -1, axis=3)
        return (times(spatial, factor), factor, carried), sums

    _, loops = lax.scan(radius, (link_x, link_x, temporal), None, length=RMAX)
    loops = lax.psum(loops, ("gx", "gy", "ta"))
    loops = lax.dynamic_slice_in_dim(loops, lax.axis_index("gx") * nx, nx, axis=2)
    loops = lax.dynamic_slice_in_dim(loops, lax.axis_index("ta") * nt, nt, axis=3)
    return loops / (3.0 * (ns * gy))


def local(link_x, link_t):
    gx, gy, ta = (lax.axis_size(a) for a in ("gx", "gy", "ta"))
    nx, nt, ns = link_x.shape[3:]
    sub = ns // (gx * ta)
    dims = (gx, gy, ta, nx, nt, ns, sub)
    fits = (
        ns == LANES
        and sub == ROWS
        and gx == nx == nt == ta == 4
    )
    return (fast if fits else general)(dims, link_x, link_t)


def solution(mesh):
    spec = P(None, None, None, "gx", "ta", "gy")
    return jax.shard_map(
        local,
        mesh=mesh,
        in_specs=(spec, spec),
        out_specs=P(None, None, "gx", "ta"),
        check_vma=False,
    )
```

```python
import contextlib
import functools

import jax
import jax.numpy as jnp
from jax import lax
from jax.experimental import pallas as pl
from jax.experimental.pallas import tpu as pltpu
from jax.sharding import PartitionSpec as P

RMAX = 6
TMAX = 6
LANES = 128
ROWS = 8
MESH = pl.DeviceIdType.MESH
scope = lambda name: contextlib.nullcontext()


def product(left, right):
    (ar, ai), (br, bi) = left, right
    real = imag = None
    for j in range(3):
        a_re, a_im = ar[:, j][:, None], ai[:, j][:, None]
        b_re, b_im = br[j][None], bi[j][None]
        re = a_re * b_re - a_im * b_im
        im = a_re * b_im + a_im * b_re
        real = re if real is None else real + re
        imag = im if imag is None else imag + im
    return real, imag


def product_dagger(left, right):
    (ar, ai), (br, bi) = left, right
    real = imag = None
    for j in range(3):
        a_re, a_im = ar[:, j][:, None], ai[:, j][:, None]
        b_re, b_im = br[:, j][None], bi[:, j][None]
        re = a_re * b_re + a_im * b_im
        im = a_im * b_re - a_re * b_im
        real = re if real is None else real + re
        imag = im if imag is None else imag + im
    return real, imag


def third(two):
    (ar, br), (ai, bi) = ((m[0], m[1]) for m in two)
    real, imag = [], []
    for k in range(3):
        p, q = (k + 1) % 3, (k + 2) % 3
        real.append(ar[p] * br[q] - ai[p] * bi[q] - ar[q] * br[p] + ai[q] * bi[p])
        imag.append(ar[q] * bi[p] + ai[q] * br[p] - ar[p] * bi[q] - ai[p] * br[q])
    return jnp.stack(real), jnp.stack(imag)


def full(two):
    return tuple(jnp.concatenate([m, t[None]], axis=0) for m, t in zip(two, third(two)))


def unit_where(mask, mat):
    rows = mat[0].shape[0]
    real = [
        jnp.stack([jnp.where(mask, mat[0][i, k], 1.0 if i == k else 0.0) for k in range(3)])
        for i in range(rows)
    ]
    return jnp.stack(real), jnp.where(mask, mat[1], 0.0)


def rolled(mat, shift, axis):
    return tuple(
        pltpu.roll(m.reshape(-1, *m.shape[2:]), shift, axis).reshape(m.shape) for m in mat
    )


def pivot(mat):
    size = [jnp.maximum(jnp.abs(mat[0][0, k]), jnp.abs(mat[1][0, k])) for k in range(3)]
    first = (size[0] >= size[1]) & (size[0] >= size[2])
    return first, size[1] >= size[2]


def choose(masks, a, b, c):
    return jnp.where(masks[0], a, jnp.where(masks[1], b, c))


def shorten(mat):
    masks = pivot(mat)
    parts = [m[0, k] for m in mat for k in range(3)]
    for m in mat:
        b = m[1]
        parts.append(choose(masks, b[1], b[2], b[0]))
        parts.append(choose(masks, b[2], b[0], b[1]))
    return parts


def lengthen(parts):
    ar, ai = parts[0:3], parts[3:6]
    (pr, qr), (pi, qi) = parts[6:8], parts[8:10]
    masks = pivot((parts[None, 0:3], parts[None, 3:6]))
    cr, ci = (choose(masks, a[0], a[1], a[2]) for a in (ar, ai))
    dr, di = (choose(masks, a[1], a[2], a[0]) for a in (ar, ai))
    er, ei = (choose(masks, a[2], a[0], a[1]) for a in (ar, ai))
    wr = dr * pr + di * pi + er * qr + ei * qi
    wi = dr * pi - di * pr + er * qi - ei * qr
    scale = -1.0 / (cr * cr + ci * ci)
    kr, ki = (wr * cr - wi * ci) * scale, (wr * ci + wi * cr) * scale
    second = []
    for k, p, q in ((kr, pr, qr), (ki, pi, qi)):
        second.append(jnp.stack([choose(masks, k, q, p), choose(masks, p, k, q), choose(masks, q, p, k)]))
    return jnp.stack([ar, second[0]]), jnp.stack([ai, second[1]])


def pair(block):
    half = block.reshape(2, -1, *block.shape[1:])
    return tuple(m.reshape(-1, 3, *block.shape[1:]) for m in half)


def flat(mat):
    return jnp.concatenate([m.reshape(-1, *m.shape[2:]) for m in mat], axis=0)


def join(early, late, sub):
    row = lax.broadcasted_iota(jnp.int32, early.shape, 1) // (ROWS // 2)
    lane = lax.broadcasted_iota(jnp.int32, early.shape, 2) // sub % 2
    early_turned, late_turned = (pltpu.roll(b, ROWS // 2, 1) for b in (early, late))
    even = jnp.where(row == 0, early, late_turned)
    odd = jnp.where(row == 0, early_turned, late)
    return jnp.where(lane == 0, even, odd)


def spread(total, nx, nt, sub, out_ref):
    shape = (nx * nt, LANES)
    corner = lax.broadcasted_iota(jnp.int32, shape, 0)
    column = lax.broadcasted_iota(jnp.int32, shape, 1)
    base = (corner // nt) * (sub * nt) + corner % nt
    for r in range(RMAX):
        first = r * TMAX // sub
        item = jnp.minimum(column + (r * TMAX - first * sub), 2 * sub - 1)
        lanes = base + item % sub * nt
        value = None
        for g in range(first, (r * TMAX + TMAX - 1) // sub + 1):
            line = jnp.broadcast_to(total[g : g + 1], shape)
            line = jnp.take_along_axis(line, lanes, axis=1)
            value = line if value is None else jnp.where(item < sub, value, line)
        out_ref[r] = value.reshape(nx, nt, LANES)[:, :, :TMAX]


def kernel(
    dims, lx_ref, lt_ref, out_ref, raw, first, block, send, recv, lines, edge, middle, step_t, trans, part,
    gath, in_sem, send_sem, recv_sem, send2_sem, recv2_sem, entered,
):
    gx, gy, ta, nx, nt, ns, sub = dims
    groups = gx * ta
    total_t = ta * nt
    mx, my, mt = lax.axis_index("gx"), lax.axis_index("gy"), lax.axis_index("ta")
    me = mt * gx + mx
    sites = nx * nt
    comps = 12
    short = 10

    inner = lax.rem((mt + 1) // 2, 2)
    opposite, second = ta - 1 - mt, lax.rem(mt + 2, ta)
    ranks = [
        mt,
        mt + 1 - 2 * lax.rem(mt, 2),
        inner * opposite + (1 - inner) * second,
        inner * second + (1 - inner) * opposite,
    ]
    steps = [(a, b, c, d) for a in range(2) for b in range(2) for c in range(gy) for d in range(ta)]
    steps = [o for o in steps if any(o)]
    plane = [o for o in steps if o[2] == 0]
    plane.sort(key=lambda o: (-o[3] * 2 - o[0] * 3, o[1]))
    steps.sort(key=lambda o: (-o[2] - o[0] - o[3], o[1]))
    peers = [o for o in steps if o[0] == o[1] == o[3] == 0]

    def target(step):
        a, b, c, d = step
        return {
            "gx": lax.rem(mx // 2 + a, 2) * 2 + lax.rem(mx + b, 2),
            "gy": lax.rem(my + c, gy),
            "ta": ranks[d],
        }

    barrier = pltpu.get_barrier_semaphore()
    for step in plane + peers:
        pl.semaphore_signal(barrier, inc=1, device_id=target(step), device_id_type=MESH)

    for f, ref in enumerate((lt_ref, lx_ref)):
        pltpu.make_async_copy(ref.at[:, pl.ds(0, 6 * sites)], raw.at[f], in_sem.at[f]).start()

    with scope("p_load"):
        pltpu.make_async_copy(raw.at[0], raw.at[0], in_sem.at[0]).wait()
    with scope("p_local"):
        t_local = lax.broadcasted_iota(jnp.int32, (sites, LANES), 0) % nt
        x_local = lax.broadcasted_iota(jnp.int32, (sites, LANES), 0) // nt
        line = pair(raw[0].reshape(comps, sites, LANES))
        step = 1
        while step < nt:
            earlier = unit_where(t_local >= step, rolled(line, step, 1))
            line = product(earlier, full(line))
            step *= 2
        first[...] = flat(line).reshape(comps * sites, LANES)
        for k in range(2):
            for m in range(3):
                for xl in range(2):
                    block[k, pl.ds(short * ROWS + m * ROWS + xl * 4, 4), :] = first[
                        pl.ds(4 * m * sites + (2 * k + xl) * nt + nt - 1, 4, stride=sites), :
                    ]
            for tt in range(2):
                block[k, pl.ds(short * ROWS + 2 * comps + tt * comps, comps), :] = first[
                    pl.ds(2 * k + tt, comps, stride=sites), :
                ]
        gauge = unit_where(t_local >= 1, rolled(line, 1, 1))
        pltpu.make_async_copy(raw.at[1], raw.at[1], in_sem.at[1]).wait()
        link = full(pair(raw[1].reshape(comps, sites, LANES)))
        beyond = unit_where(x_local < nx - 1, rolled(full(gauge), sites - nt, 1))
        parts = shorten(product_dagger(product(gauge, link), beyond))
        for k in range(2):
            for c in range(short):
                block[k, pl.ds(c * ROWS, ROWS), :] = parts[c][k * ROWS : (k + 1) * ROWS]
            send[:, pl.ds(k * sub, sub), :] = block[k].T.reshape(groups, sub, LANES)

    with scope("p_bar"):
        pl.semaphore_wait(barrier, len(plane + peers))
    for step in peers:
        pl.semaphore_signal(entered, inc=1, device_id=target(step), device_id_type=MESH)

    for step in plane:
        where = target(step)
        pltpu.make_async_remote_copy(
            src_ref=send.at[where["ta"] * gx + where["gx"]],
            dst_ref=recv.at[me],
            send_sem=send_sem,
            recv_sem=recv_sem.at[mt // 2],
            device_id=where,
            device_id_type=MESH,
        ).start()
    own = pltpu.make_async_copy(send.at[me], recv.at[me], recv_sem.at[mt // 2])
    own.start()

    def next_x(mat):
        return tuple(
            pltpu.roll(m.reshape(-1, LANES), LANES - sub, 1).reshape(m.shape) for m in mat
        )

    t_half = lax.broadcasted_iota(jnp.int32, (ROWS, LANES), 0) % nt
    x_lane = lax.broadcasted_iota(jnp.int32, (ROWS, LANES), 1) // sub % nx
    for order in range(2):
        half = lax.rem(mt // 2 + order, 2)
        landed = recv.at[pl.ds(half * 2 * gx, 2 * gx)]
        with scope(f"p_w{order}"):
            pltpu.make_async_copy(landed, landed, recv_sem.at[half]).wait()
        with scope(f"p_half{order}"):
            got = recv[pl.ds(half * 2 * gx, 2 * gx)].reshape(2, gx * 2, sub, LANES)
            got = [jnp.stack([got[td], got[td]], axis=1).reshape(LANES, LANES).T for td in range(2)]
            cuts = short * ROWS, short * ROWS + 2 * comps
            parts = join(*(g[: cuts[0]].reshape(short, ROWS, LANES) for g in got), sub)
            ends = join(*(g[cuts[0] : cuts[1]].reshape(3, ROWS, LANES) for g in got), sub)
            for m in range(3):
                for td in range(2):
                    lines[pl.ds(4 * m * ROWS + half * 2 + td + 1, 4, stride=ROWS), :] = ends[m, td * 4 : td * 4 + 4]
            for td in range(2):
                near = pltpu.roll(got[td][cuts[1] :], LANES - sub, 1)
                far = pltpu.roll(got[td][cuts[1] : cuts[1] + 2 * ROWS], LANES - 3 * sub, 1)
                edge[pl.ds(td * nt + 1, comps, stride=ROWS), :] = near[:comps]
                edge[pl.ds(td * nt + 2, comps, stride=ROWS), :] = near[comps:]
                edge[pl.ds(td * nt + 3, comps, stride=ROWS), :] = far[:comps]
            end = pair(edge[...].reshape(comps, ROWS, LANES))
            end = full(unit_where((t_half > 0) & (x_lane == nx - 1), end))
            middle[:, pl.ds(half * ROWS, ROWS), :] = flat(product_dagger(lengthen(parts), end))

    with scope("p_prefix"):
        row = lax.broadcasted_iota(jnp.int32, (ROWS, LANES), 0)
        hop = lines[...].reshape(comps, ROWS, LANES)
        hop = jnp.where(row == ta + 1, pltpu.roll(hop, ta, 1), hop)
        hop = unit_where((row > 0) & (row < ta + 2), pair(hop))
        step = 1
        while step < ta + 2:
            earlier = unit_where(row >= step, rolled(hop, step, 1))
            hop = product(earlier, full(hop))
            step *= 2
        hop = full(hop)
        step_t[0] = flat(hop).reshape(18 * ROWS, LANES)
        step_t[1] = flat(next_x(hop)).reshape(18 * ROWS, LANES)

    def spread_t(side, rows, v):
        out = []
        for c in range(18):
            if c % 9 >= 3 * rows:
                continue
            low, high = (
                jnp.broadcast_to(step_t[side, pl.ds(c * ROWS + 2 * v + td, 1), :], (ROWS, LANES))
                for td in range(2)
            )
            out.append(jnp.where(row < nt, low, high))
        return pair(jnp.stack(out))

    row_t = row // nt
    lane = lax.broadcasted_iota(jnp.int32, (ROWS, LANES), 1)
    block_x = lane // (LANES // nx)
    own_time = row % nt * (LANES // nx) + lane % (LANES // nx)

    def emit(items, g, held):
        stack = []
        for td in range(ta):
            for a, b in zip(items[::2], items[1::2]):
                a, b = a[td // 2], b[td // 2]
                if td % 2:
                    stack.append(jnp.where(row_t == 0, pltpu.roll(a, nt, 0), b))
                else:
                    stack.append(jnp.where(row_t == 0, a, pltpu.roll(b, nt, 0)))
            stack += [jnp.zeros((ROWS, LANES), jnp.float32)] * ((sub - len(items)) // 2)
        turned = jnp.concatenate(stack, axis=0).T.reshape(gx * nx, sub, LANES)
        for step in (4, 2, 1):
            turned = turned + pltpu.roll(turned, step, 1)
        if g % 2 == 0 and g < rows - 1:
            return turned
        low = turned if held is None else held
        for j in range(gx):
            value = None
            for x in range(nx):
                both = jnp.where(row_t == 0, low[j * nx + x], turned[j * nx + x])
                both = jnp.take_along_axis(both, own_time, axis=1)
                value = both if value is None else jnp.where(block_x == x, both, value)
            for k in range(1 if held is None else 2):
                part[pl.ds(j * ROWS + g // 2 * 2 + k, ta, stride=gx * ROWS), :] = value[k * nt : k * nt + ta]
        return None

    rows = -(-RMAX * TMAX // sub)
    with scope("p_path"):
        for v in range(total_t // ROWS + 1):
            start = v * ROWS
            inner = pair(middle[:, pl.ds(start % total_t, ROWS), :])
            moved = product(spread_t(0, 2, v), full(product_dagger(inner, spread_t(1, 3, v))))
            trans[0, :, pl.ds(start, ROWS), :] = flat(full(moved))
    with scope("p_sums"):
        items, g, held = [], 0, None
        for r in range(RMAX):
            for v in range(total_t // ROWS + 1) if r else ():
                here = pl.ds(v * ROWS, ROWS)
                moved = pair(pltpu.roll(trans[0, :, here, :].reshape(-1, LANES), LANES - r * sub, 1).reshape(18, ROWS, LANES))
                path = pair(trans[r - 1, :, here, :])
                path = product((path[0][:2], path[1][:2]), moved)
                trans[r, :, here, :] = flat(full(path))
            for u in range(1, TMAX + 1):
                items.append(
                    [
                        jnp.sum(trans[r, :, pl.ds(start, ROWS), :] * trans[r, :, pl.ds(start + u, ROWS), :], axis=0)
                        for start in range(0, total_t, ROWS)
                    ]
                )
                if len(items) == sub or (r, u) == (RMAX - 1, TMAX):
                    held = emit(items, g, held)
                    items, g = [], g + 1

    slot = my * groups + me
    with scope("p_entered"):
        pl.semaphore_wait(entered, len(peers))
    with scope("p_send2"):
        for step in steps:
            where = target(step)
            pltpu.make_async_remote_copy(
                src_ref=part.at[pl.ds((where["ta"] * gx + where["gx"]) * ROWS, rows)],
                dst_ref=gath.at[slot],
                send_sem=send2_sem,
                recv_sem=recv2_sem,
                device_id=where,
                device_id_type=MESH,
            ).start()
    gath[slot] = part[pl.ds(me * ROWS, rows), :]
    with scope("p_wait2"):
        sent = send.at[pl.ds(0, len(plane))]
        pltpu.make_async_copy(sent, sent, send_sem).wait()
        landed = gath.at[pl.ds(0, len(steps))]
        pltpu.make_async_copy(landed, landed, send2_sem).wait()
        pltpu.make_async_copy(landed, landed, recv2_sem).wait()
    spread(jnp.sum(gath[...], axis=0) / (3.0 * (ns * gy)), nx, nt, sub, out_ref)


def fast(dims, link_x, link_t):
    gx, gy, ta, nx, nt, ns, sub = dims
    groups = gx * ta
    total_t = ta * nt
    flat = (2, 9 * nx * nt, ns)
    rows = -(-RMAX * TMAX // sub)
    out = pl.pallas_call(
        functools.partial(kernel, dims),
        out_shape=pltpu.VMEM((RMAX, nx, nt, TMAX), jnp.float32),
        in_specs=[pl.BlockSpec(memory_space=pl.ANY)] * 2,
        out_specs=pl.BlockSpec(memory_space=pltpu.VMEM),
        scratch_shapes=[
            pltpu.VMEM((2, 2, 6 * nx * nt, ns), jnp.float32),
            pltpu.VMEM((12 * nx * nt, ns), jnp.float32),
            pltpu.VMEM((2, LANES, ns), jnp.float32),
            pltpu.VMEM((groups, 2 * sub, LANES), jnp.float32),
            pltpu.VMEM((groups, 2 * sub, LANES), jnp.float32),
            pltpu.VMEM((12 * ROWS, LANES), jnp.float32),
            pltpu.VMEM((12 * ROWS, LANES), jnp.float32),
            pltpu.VMEM((12, total_t, LANES), jnp.float32),
            pltpu.VMEM((2, 18 * ROWS, LANES), jnp.float32),
            pltpu.VMEM((RMAX, 18, total_t + ROWS, LANES), jnp.float32),
            pltpu.VMEM((groups * ROWS, LANES), jnp.float32),
            pltpu.VMEM((gy * groups, rows, LANES), jnp.float32),
            pltpu.SemaphoreType.DMA((2,)),
            pltpu.SemaphoreType.DMA,
            pltpu.SemaphoreType.DMA((2,)),
            pltpu.SemaphoreType.DMA,
            pltpu.SemaphoreType.DMA,
            pltpu.SemaphoreType.REGULAR,
        ],
        compiler_params=pltpu.CompilerParams(collective_id=0, has_side_effects=True),
        name="wilson",
    )(link_x.reshape(flat), link_t.reshape(flat))
    return out.transpose(0, 3, 1, 2)


def times(left, right):
    def dot(a, b):
        return sum(a[:, j][:, None] * b[j][None] for j in range(3))

    real = dot(left[0], right[0]) - dot(left[1], right[1])
    imag = dot(left[0], right[1]) + dot(left[1], right[0])
    return jnp.stack([real, imag])


def general(dims, link_x, link_t):
    gx, gy, ta, nx, nt, ns, sub = dims

    def gather(field):
        field = lax.all_to_all(field, "gx", 5, 3, tiled=True)
        return lax.all_to_all(field, "ta", 5, 4, tiled=True)

    link_x, link_t = gather(link_x), gather(link_t)

    def grow_t(carry, _):
        line, factor = carry
        factor = jnp.roll(factor, -1, axis=4)
        return (times(line, factor), factor), line

    _, temporal = lax.scan(grow_t, (link_t, link_t), None, length=TMAX)

    def radius(carry, _):
        spatial, factor, carried = carry
        carried = jnp.roll(carried, -1, axis=4)

        def extent(shifted, pair):
            line, line_r = pair
            shifted = jnp.roll(shifted, -1, axis=4)
            return shifted, jnp.sum(times(spatial, line_r) * times(line, shifted), axis=(0, 1, 2, 5))

        _, sums = lax.scan(extent, spatial, (temporal, carried))
        factor = jnp.roll(factor, -1, axis=3)
        return (times(spatial, factor), factor, carried), sums

    _, loops = lax.scan(radius, (link_x, link_x, temporal), None, length=RMAX)
    loops = lax.psum(loops, ("gx", "gy", "ta"))
    loops = lax.dynamic_slice_in_dim(loops, lax.axis_index("gx") * nx, nx, axis=2)
    loops = lax.dynamic_slice_in_dim(loops, lax.axis_index("ta") * nt, nt, axis=3)
    return loops / (3.0 * (ns * gy))


def local(link_x, link_t):
    gx, gy, ta = (lax.axis_size(a) for a in ("gx", "gy", "ta"))
    nx, nt, ns = link_x.shape[3:]
    sub = ns // (gx * ta)
    dims = (gx, gy, ta, nx, nt, ns, sub)
    fits = (
        ns == LANES
        and sub == ROWS
        and gx == nx == nt == ta == 4
    )
    return (fast if fits else general)(dims, link_x, link_t)


def solution(mesh):
    spec = P(None, None, None, "gx", "ta", "gy")
    return jax.shard_map(
        local,
        mesh=mesh,
        in_specs=(spec, spec),
        out_specs=P(None, None, "gx", "ta"),
        check_vma=False,
    )
```

```python
import contextlib
import functools

import jax
import jax.numpy as jnp
from jax import lax
from jax.experimental import pallas as pl
from jax.experimental.pallas import tpu as pltpu
from jax.sharding import PartitionSpec as P

RMAX = 6
TMAX = 6
LANES = 128
ROWS = 8
MESH = pl.DeviceIdType.MESH
scope = lambda name: contextlib.nullcontext()


def product(left, right):
    (ar, ai), (br, bi) = left, right
    real = imag = None
    for j in range(3):
        a_re, a_im = ar[:, j][:, None], ai[:, j][:, None]
        b_re, b_im = br[j][None], bi[j][None]
        re = a_re * b_re - a_im * b_im
        im = a_re * b_im + a_im * b_re
        real = re if real is None else real + re
        imag = im if imag is None else imag + im
    return real, imag


def product_dagger(left, right):
    (ar, ai), (br, bi) = left, right
    real = imag = None
    for j in range(3):
        a_re, a_im = ar[:, j][:, None], ai[:, j][:, None]
        b_re, b_im = br[:, j][None], bi[:, j][None]
        re = a_re * b_re + a_im * b_im
        im = a_im * b_re - a_re * b_im
        real = re if real is None else real + re
        imag = im if imag is None else imag + im
    return real, imag


def third(two):
    (ar, br), (ai, bi) = ((m[0], m[1]) for m in two)
    real, imag = [], []
    for k in range(3):
        p, q = (k + 1) % 3, (k + 2) % 3
        real.append(ar[p] * br[q] - ai[p] * bi[q] - ar[q] * br[p] + ai[q] * bi[p])
        imag.append(ar[q] * bi[p] + ai[q] * br[p] - ar[p] * bi[q] - ai[p] * br[q])
    return jnp.stack(real), jnp.stack(imag)


def full(two):
    return tuple(jnp.concatenate([m, t[None]], axis=0) for m, t in zip(two, third(two)))


def unit_where(mask, mat):
    rows = mat[0].shape[0]
    real = [
        jnp.stack([jnp.where(mask, mat[0][i, k], 1.0 if i == k else 0.0) for k in range(3)])
        for i in range(rows)
    ]
    return jnp.stack(real), jnp.where(mask, mat[1], 0.0)


def rolled(mat, shift, axis):
    return tuple(
        pltpu.roll(m.reshape(-1, *m.shape[2:]), shift, axis).reshape(m.shape) for m in mat
    )


def pivot(mat):
    size = [jnp.maximum(jnp.abs(mat[0][0, k]), jnp.abs(mat[1][0, k])) for k in range(3)]
    first = (size[0] >= size[1]) & (size[0] >= size[2])
    return first, size[1] >= size[2]


def choose(masks, a, b, c):
    return jnp.where(masks[0], a, jnp.where(masks[1], b, c))


def shorten(mat):
    masks = pivot(mat)
    parts = [m[0, k] for m in mat for k in range(3)]
    for m in mat:
        b = m[1]
        parts.append(choose(masks, b[1], b[2], b[0]))
        parts.append(choose(masks, b[2], b[0], b[1]))
    return parts


def lengthen(parts):
    ar, ai = parts[0:3], parts[3:6]
    (pr, qr), (pi, qi) = parts[6:8], parts[8:10]
    masks = pivot((parts[None, 0:3], parts[None, 3:6]))
    cr, ci = (choose(masks, a[0], a[1], a[2]) for a in (ar, ai))
    dr, di = (choose(masks, a[1], a[2], a[0]) for a in (ar, ai))
    er, ei = (choose(masks, a[2], a[0], a[1]) for a in (ar, ai))
    wr = dr * pr + di * pi + er * qr + ei * qi
    wi = dr * pi - di * pr + er * qi - ei * qr
    scale = -1.0 / (cr * cr + ci * ci)
    kr, ki = (wr * cr - wi * ci) * scale, (wr * ci + wi * cr) * scale
    second = []
    for k, p, q in ((kr, pr, qr), (ki, pi, qi)):
        second.append(jnp.stack([choose(masks, k, q, p), choose(masks, p, k, q), choose(masks, q, p, k)]))
    return jnp.stack([ar, second[0]]), jnp.stack([ai, second[1]])


def pair(block):
    half = block.reshape(2, -1, *block.shape[1:])
    return tuple(m.reshape(-1, 3, *block.shape[1:]) for m in half)


def flat(mat):
    return jnp.concatenate([m.reshape(-1, *m.shape[2:]) for m in mat], axis=0)


def join(early, late, sub):
    row = lax.broadcasted_iota(jnp.int32, early.shape, 1) // (ROWS // 2)
    lane = lax.broadcasted_iota(jnp.int32, early.shape, 2) // sub % 2
    early_turned, late_turned = (pltpu.roll(b, ROWS // 2, 1) for b in (early, late))
    even = jnp.where(row == 0, early, late_turned)
    odd = jnp.where(row == 0, early_turned, late)
    return jnp.where(lane == 0, even, odd)


def spread(total, nx, nt, sub, out_ref):
    shape = (nx * nt, LANES)
    corner = lax.broadcasted_iota(jnp.int32, shape, 0)
    column = lax.broadcasted_iota(jnp.int32, shape, 1)
    base = (corner // nt) * (sub * nt) + corner % nt
    for r in range(RMAX):
        first = r * TMAX // sub
        item = jnp.minimum(column + (r * TMAX - first * sub), 2 * sub - 1)
        lanes = base + item % sub * nt
        value = None
        for g in range(first, (r * TMAX + TMAX - 1) // sub + 1):
            line = jnp.broadcast_to(total[g : g + 1], shape)
            line = jnp.take_along_axis(line, lanes, axis=1)
            value = line if value is None else jnp.where(item < sub, value, line)
        out_ref[r] = value.reshape(nx, nt, LANES)[:, :, :TMAX]


def kernel(
    dims, lx_ref, lt_ref, out_ref, raw, first, block, send, recv, lines, edge, middle, step_t, trans, part,
    gath, in_sem, send_sem, recv_sem, send2_sem, recv2_sem, entered,
):
    gx, gy, ta, nx, nt, ns, sub = dims
    groups = gx * ta
    total_t = ta * nt
    mx, my, mt = lax.axis_index("gx"), lax.axis_index("gy"), lax.axis_index("ta")
    me = mt * gx + mx
    sites = nx * nt
    comps = 12
    short = 10

    inner = lax.rem((mt + 1) // 2, 2)
    opposite, second = ta - 1 - mt, lax.rem(mt + 2, ta)
    ranks = [
        mt,
        mt + 1 - 2 * lax.rem(mt, 2),
        inner * opposite + (1 - inner) * second,
        inner * second + (1 - inner) * opposite,
    ]
    steps = [(a, b, c, d) for a in range(2) for b in range(2) for c in range(gy) for d in range(ta)]
    steps = [o for o in steps if any(o)]
    plane = [o for o in steps if o[2] == 0]
    plane.sort(key=lambda o: (-o[3] * 2 - o[0] * 3, o[1]))
    steps.sort(key=lambda o: (-o[2] - o[0] - o[3], o[1]))
    peers = [o for o in steps if o[0] == o[1] == o[3] == 0]

    def target(step):
        a, b, c, d = step
        return {
            "gx": lax.rem(mx // 2 + a, 2) * 2 + lax.rem(mx + b, 2),
            "gy": lax.rem(my + c, gy),
            "ta": ranks[d],
        }

    barrier = pltpu.get_barrier_semaphore()
    for step in plane + peers:
        pl.semaphore_signal(barrier, inc=1, device_id=target(step), device_id_type=MESH)

    for f, ref in enumerate((lt_ref, lx_ref)):
        for c in range(2):
            pltpu.make_async_copy(
                ref.at[c, pl.ds(0, 6 * sites)], raw.at[f, pl.ds(c * 6 * sites, 6 * sites)], in_sem.at[f]
            ).start()

    with scope("p_load"):
        pltpu.make_async_copy(raw.at[0], raw.at[0], in_sem.at[0]).wait()
    with scope("p_local"):
        t_local = lax.broadcasted_iota(jnp.int32, (sites, LANES), 0) % nt
        x_local = lax.broadcasted_iota(jnp.int32, (sites, LANES), 0) // nt
        line = pair(raw[0].reshape(comps, sites, LANES))
        step = 1
        while step < nt:
            earlier = unit_where(t_local >= step, rolled(line, step, 1))
            line = product(earlier, full(line))
            step *= 2
        first[...] = flat(line).reshape(comps * sites, LANES)
        for k in range(2):
            for m in range(3):
                for xl in range(2):
                    block[k, pl.ds(short * ROWS + m * ROWS + xl * 4, 4), :] = first[
                        pl.ds(4 * m * sites + (2 * k + xl) * nt + nt - 1, 4, stride=sites), :
                    ]
            for tt in range(2):
                block[k, pl.ds(short * ROWS + 2 * comps + tt * comps, comps), :] = first[
                    pl.ds(2 * k + tt, comps, stride=sites), :
                ]
        gauge = unit_where(t_local >= 1, rolled(line, 1, 1))
        pltpu.make_async_copy(raw.at[1], raw.at[1], in_sem.at[1]).wait()
        link = full(pair(raw[1].reshape(comps, sites, LANES)))
        beyond = unit_where(x_local < nx - 1, rolled(full(gauge), sites - nt, 1))
        parts = shorten(product_dagger(product(gauge, link), beyond))
        for k in range(2):
            for c in range(short):
                block[k, pl.ds(c * ROWS, ROWS), :] = parts[c][k * ROWS : (k + 1) * ROWS]
            send[:, pl.ds(k * sub, sub), :] = block[k].T.reshape(groups, sub, LANES)

    with scope("p_bar"):
        pl.semaphore_wait(barrier, len(plane + peers))
    for step in peers:
        pl.semaphore_signal(entered, inc=1, device_id=target(step), device_id_type=MESH)

    for step in plane:
        where = target(step)
        pltpu.make_async_remote_copy(
            src_ref=send.at[where["ta"] * gx + where["gx"]],
            dst_ref=recv.at[me],
            send_sem=send_sem,
            recv_sem=recv_sem.at[mt // 2],
            device_id=where,
            device_id_type=MESH,
        ).start()
    own = pltpu.make_async_copy(send.at[me], recv.at[me], recv_sem.at[mt // 2])
    own.start()

    def next_x(mat):
        return tuple(
            pltpu.roll(m.reshape(-1, LANES), LANES - sub, 1).reshape(m.shape) for m in mat
        )

    t_half = lax.broadcasted_iota(jnp.int32, (ROWS, LANES), 0) % nt
    x_lane = lax.broadcasted_iota(jnp.int32, (ROWS, LANES), 1) // sub % nx
    for order in range(2):
        half = lax.rem(mt // 2 + order, 2)
        landed = recv.at[pl.ds(half * 2 * gx, 2 * gx)]
        with scope(f"p_w{order}"):
            pltpu.make_async_copy(landed, landed, recv_sem.at[half]).wait()
        with scope(f"p_half{order}"):
            got = recv[pl.ds(half * 2 * gx, 2 * gx)].reshape(2, gx * 2, sub, LANES)
            got = [jnp.stack([got[td], got[td]], axis=1).reshape(LANES, LANES).T for td in range(2)]
            cuts = short * ROWS, short * ROWS + 2 * comps
            parts = join(*(g[: cuts[0]].reshape(short, ROWS, LANES) for g in got), sub)
            ends = join(*(g[cuts[0] : cuts[1]].reshape(3, ROWS, LANES) for g in got), sub)
            for m in range(3):
                for td in range(2):
                    lines[pl.ds(4 * m * ROWS + half * 2 + td + 1, 4, stride=ROWS), :] = ends[m, td * 4 : td * 4 + 4]
            for td in range(2):
                near = pltpu.roll(got[td][cuts[1] :], LANES - sub, 1)
                far = pltpu.roll(got[td][cuts[1] : cuts[1] + 2 * ROWS], LANES - 3 * sub, 1)
                edge[pl.ds(td * nt + 1, comps, stride=ROWS), :] = near[:comps]
                edge[pl.ds(td * nt + 2, comps, stride=ROWS), :] = near[comps:]
                edge[pl.ds(td * nt + 3, comps, stride=ROWS), :] = far[:comps]
            end = pair(edge[...].reshape(comps, ROWS, LANES))
            end = full(unit_where((t_half > 0) & (x_lane == nx - 1), end))
            middle[:, pl.ds(half * ROWS, ROWS), :] = flat(product_dagger(lengthen(parts), end))

    with scope("p_prefix"):
        row = lax.broadcasted_iota(jnp.int32, (ROWS, LANES), 0)
        hop = lines[...].reshape(comps, ROWS, LANES)
        hop = jnp.where(row == ta + 1, pltpu.roll(hop, ta, 1), hop)
        hop = unit_where((row > 0) & (row < ta + 2), pair(hop))
        step = 1
        while step < ta + 2:
            earlier = unit_where(row >= step, rolled(hop, step, 1))
            hop = product(earlier, full(hop))
            step *= 2
        hop = full(hop)
        step_t[0] = flat(hop).reshape(18 * ROWS, LANES)
        step_t[1] = flat(next_x(hop)).reshape(18 * ROWS, LANES)

    def spread_t(side, rows, v):
        out = []
        for c in range(18):
            if c % 9 >= 3 * rows:
                continue
            low, high = (
                jnp.broadcast_to(step_t[side, pl.ds(c * ROWS + 2 * v + td, 1), :], (ROWS, LANES))
                for td in range(2)
            )
            out.append(jnp.where(row < nt, low, high))
        return pair(jnp.stack(out))

    row_t = row // nt
    lane = lax.broadcasted_iota(jnp.int32, (ROWS, LANES), 1)
    block_x = lane // (LANES // nx)
    own_time = row % nt * (LANES // nx) + lane % (LANES // nx)

    def emit(items, g, held):
        stack = []
        for td in range(ta):
            for a, b in zip(items[::2], items[1::2]):
                a, b = a[td // 2], b[td // 2]
                if td % 2:
                    stack.append(jnp.where(row_t == 0, pltpu.roll(a, nt, 0), b))
                else:
                    stack.append(jnp.where(row_t == 0, a, pltpu.roll(b, nt, 0)))
            stack += [jnp.zeros((ROWS, LANES), jnp.float32)] * ((sub - len(items)) // 2)
        turned = jnp.concatenate(stack, axis=0).T.reshape(gx * nx, sub, LANES)
        for step in (4, 2, 1):
            turned = turned + pltpu.roll(turned, step, 1)
        if g % 2 == 0 and g < rows - 1:
            return turned
        low = turned if held is None else held
        for j in range(gx):
            value = None
            for x in range(nx):
                both = jnp.where(row_t == 0, low[j * nx + x], turned[j * nx + x])
                both = jnp.take_along_axis(both, own_time, axis=1)
                value = both if value is None else jnp.where(block_x == x, both, value)
            for k in range(1 if held is None else 2):
                part[pl.ds(j * ROWS + g // 2 * 2 + k, ta, stride=gx * ROWS), :] = value[k * nt : k * nt + ta]
        return None

    rows = -(-RMAX * TMAX // sub)
    with scope("p_path"):
        for v in range(total_t // ROWS + 1):
            start = v * ROWS
            inner = pair(middle[:, pl.ds(start % total_t, ROWS), :])
            moved = product(spread_t(0, 2, v), full(product_dagger(inner, spread_t(1, 3, v))))
            trans[0, :, pl.ds(start, ROWS), :] = flat(full(moved))
    with scope("p_sums"):
        items, g, held = [], 0, None
        for r in range(RMAX):
            for v in range(total_t // ROWS + 1) if r else ():
                here = pl.ds(v * ROWS, ROWS)
                moved = pair(pltpu.roll(trans[0, :, here, :].reshape(-1, LANES), LANES - r * sub, 1).reshape(18, ROWS, LANES))
                path = pair(trans[r - 1, :, here, :])
                path = product((path[0][:2], path[1][:2]), moved)
                trans[r, :, here, :] = flat(full(path))
            for u in range(1, TMAX + 1):
                items.append(
                    [
                        jnp.sum(trans[r, :, pl.ds(start, ROWS), :] * trans[r, :, pl.ds(start + u, ROWS), :], axis=0)
                        for start in range(0, total_t, ROWS)
                    ]
                )
                if len(items) == sub or (r, u) == (RMAX - 1, TMAX):
                    held = emit(items, g, held)
                    items, g = [], g + 1

    slot = my * groups + me
    with scope("p_entered"):
        pl.semaphore_wait(entered, len(peers))
    with scope("p_send2"):
        for step in steps:
            where = target(step)
            pltpu.make_async_remote_copy(
                src_ref=part.at[pl.ds((where["ta"] * gx + where["gx"]) * ROWS, rows)],
                dst_ref=gath.at[slot],
                send_sem=send2_sem,
                recv_sem=recv2_sem,
                device_id=where,
                device_id_type=MESH,
            ).start()
    gath[slot] = part[pl.ds(me * ROWS, rows), :]
    with scope("p_wait2"):
        sent = send.at[pl.ds(0, len(plane))]
        pltpu.make_async_copy(sent, sent, send_sem).wait()
        landed = gath.at[pl.ds(0, len(steps))]
        pltpu.make_async_copy(landed, landed, send2_sem).wait()
        pltpu.make_async_copy(landed, landed, recv2_sem).wait()
    total = [gath[k] for k in range(gy * groups)]
    while len(total) > 1:
        total = [sum(total[k : k + 2]) for k in range(0, len(total), 2)]
    spread(total[0] * (1.0 / (3.0 * (ns * gy))), nx, nt, sub, out_ref)


def fast(dims, link_x, link_t):
    gx, gy, ta, nx, nt, ns, sub = dims
    groups = gx * ta
    total_t = ta * nt
    flat = (2, 9 * nx * nt, ns)
    rows = -(-RMAX * TMAX // sub)
    out = pl.pallas_call(
        functools.partial(kernel, dims),
        out_shape=pltpu.VMEM((RMAX, nx, nt, TMAX), jnp.float32),
        in_specs=[pl.BlockSpec(memory_space=pl.ANY)] * 2,
        out_specs=pl.BlockSpec(memory_space=pltpu.VMEM),
        scratch_shapes=[
            pltpu.VMEM((2, 12 * nx * nt, ns), jnp.float32),
            pltpu.VMEM((12 * nx * nt, ns), jnp.float32),
            pltpu.VMEM((2, LANES, ns), jnp.float32),
            pltpu.VMEM((groups, 2 * sub, LANES), jnp.float32),
            pltpu.VMEM((groups, 2 * sub, LANES), jnp.float32),
            pltpu.VMEM((12 * ROWS, LANES), jnp.float32),
            pltpu.VMEM((12 * ROWS, LANES), jnp.float32),
            pltpu.VMEM((12, total_t, LANES), jnp.float32),
            pltpu.VMEM((2, 18 * ROWS, LANES), jnp.float32),
            pltpu.VMEM((RMAX, 18, total_t + ROWS, LANES), jnp.float32),
            pltpu.VMEM((groups * ROWS, LANES), jnp.float32),
            pltpu.VMEM((gy * groups, rows, LANES), jnp.float32),
            pltpu.SemaphoreType.DMA((2,)),
            pltpu.SemaphoreType.DMA,
            pltpu.SemaphoreType.DMA((2,)),
            pltpu.SemaphoreType.DMA,
            pltpu.SemaphoreType.DMA,
            pltpu.SemaphoreType.REGULAR,
        ],
        compiler_params=pltpu.CompilerParams(collective_id=0, has_side_effects=True),
        name="wilson",
    )(link_x.reshape(flat), link_t.reshape(flat))
    return out.transpose(0, 3, 1, 2)


def times(left, right):
    def dot(a, b):
        return sum(a[:, j][:, None] * b[j][None] for j in range(3))

    real = dot(left[0], right[0]) - dot(left[1], right[1])
    imag = dot(left[0], right[1]) + dot(left[1], right[0])
    return jnp.stack([real, imag])


def general(dims, link_x, link_t):
    gx, gy, ta, nx, nt, ns, sub = dims

    def gather(field):
        field = lax.all_to_all(field, "gx", 5, 3, tiled=True)
        return lax.all_to_all(field, "ta", 5, 4, tiled=True)

    link_x, link_t = gather(link_x), gather(link_t)

    def grow_t(carry, _):
        line, factor = carry
        factor = jnp.roll(factor, -1, axis=4)
        return (times(line, factor), factor), line

    _, temporal = lax.scan(grow_t, (link_t, link_t), None, length=TMAX)

    def radius(carry, _):
        spatial, factor, carried = carry
        carried = jnp.roll(carried, -1, axis=4)

        def extent(shifted, pair):
            line, line_r = pair
            shifted = jnp.roll(shifted, -1, axis=4)
            return shifted, jnp.sum(times(spatial, line_r) * times(line, shifted), axis=(0, 1, 2, 5))

        _, sums = lax.scan(extent, spatial, (temporal, carried))
        factor = jnp.roll(factor, -1, axis=3)
        return (times(spatial, factor), factor, carried), sums

    _, loops = lax.scan(radius, (link_x, link_x, temporal), None, length=RMAX)
    loops = lax.psum(loops, ("gx", "gy", "ta"))
    loops = lax.dynamic_slice_in_dim(loops, lax.axis_index("gx") * nx, nx, axis=2)
    loops = lax.dynamic_slice_in_dim(loops, lax.axis_index("ta") * nt, nt, axis=3)
    return loops / (3.0 * (ns * gy))


def local(link_x, link_t):
    gx, gy, ta = (lax.axis_size(a) for a in ("gx", "gy", "ta"))
    nx, nt, ns = link_x.shape[3:]
    sub = ns // (gx * ta)
    dims = (gx, gy, ta, nx, nt, ns, sub)
    fits = (
        ns == LANES
        and sub == ROWS
        and gx == nx == nt == ta == 4
    )
    return (fast if fits else general)(dims, link_x, link_t)


def solution(mesh):
    spec = P(None, None, None, "gx", "ta", "gy")
    return jax.shard_map(
        local,
        mesh=mesh,
        in_specs=(spec, spec),
        out_specs=P(None, None, "gx", "ta"),
        check_vma=False,
    )
```

```python
import contextlib
import functools

import jax
import jax.numpy as jnp
from jax import lax
from jax.experimental import pallas as pl
from jax.experimental.pallas import tpu as pltpu
from jax.sharding import PartitionSpec as P

RMAX = 6
TMAX = 6
LANES = 128
ROWS = 8
MESH = pl.DeviceIdType.MESH
scope = lambda name: contextlib.nullcontext()


def product(left, right):
    (ar, ai), (br, bi) = left, right
    real = imag = None
    for j in range(3):
        a_re, a_im = ar[:, j][:, None], ai[:, j][:, None]
        b_re, b_im = br[j][None], bi[j][None]
        re = a_re * b_re - a_im * b_im
        im = a_re * b_im + a_im * b_re
        real = re if real is None else real + re
        imag = im if imag is None else imag + im
    return real, imag


def product_dagger(left, right):
    (ar, ai), (br, bi) = left, right
    real = imag = None
    for j in range(3):
        a_re, a_im = ar[:, j][:, None], ai[:, j][:, None]
        b_re, b_im = br[:, j][None], bi[:, j][None]
        re = a_re * b_re + a_im * b_im
        im = a_im * b_re - a_re * b_im
        real = re if real is None else real + re
        imag = im if imag is None else imag + im
    return real, imag


def third(two):
    (ar, br), (ai, bi) = ((m[0], m[1]) for m in two)
    real, imag = [], []
    for k in range(3):
        p, q = (k + 1) % 3, (k + 2) % 3
        real.append(ar[p] * br[q] - ai[p] * bi[q] - ar[q] * br[p] + ai[q] * bi[p])
        imag.append(ar[q] * bi[p] + ai[q] * br[p] - ar[p] * bi[q] - ai[p] * br[q])
    return jnp.stack(real), jnp.stack(imag)


def full(two):
    return tuple(jnp.concatenate([m, t[None]], axis=0) for m, t in zip(two, third(two)))


def unit_where(mask, mat):
    rows = mat[0].shape[0]
    real = [
        jnp.stack([jnp.where(mask, mat[0][i, k], 1.0 if i == k else 0.0) for k in range(3)])
        for i in range(rows)
    ]
    return jnp.stack(real), jnp.where(mask, mat[1], 0.0)


def rolled(mat, shift, axis):
    return tuple(
        pltpu.roll(m.reshape(-1, *m.shape[2:]), shift, axis).reshape(m.shape) for m in mat
    )


def pivot(mat):
    size = [jnp.maximum(jnp.abs(mat[0][0, k]), jnp.abs(mat[1][0, k])) for k in range(3)]
    first = (size[0] >= size[1]) & (size[0] >= size[2])
    return first, size[1] >= size[2]


def choose(masks, a, b, c):
    return jnp.where(masks[0], a, jnp.where(masks[1], b, c))


def shorten(mat):
    masks = pivot(mat)
    parts = [m[0, k] for m in mat for k in range(3)]
    for m in mat:
        b = m[1]
        parts.append(choose(masks, b[1], b[2], b[0]))
        parts.append(choose(masks, b[2], b[0], b[1]))
    return parts


def lengthen(parts):
    ar, ai = parts[0:3], parts[3:6]
    (pr, qr), (pi, qi) = parts[6:8], parts[8:10]
    masks = pivot((parts[None, 0:3], parts[None, 3:6]))
    cr, ci = (choose(masks, a[0], a[1], a[2]) for a in (ar, ai))
    dr, di = (choose(masks, a[1], a[2], a[0]) for a in (ar, ai))
    er, ei = (choose(masks, a[2], a[0], a[1]) for a in (ar, ai))
    wr = dr * pr + di * pi + er * qr + ei * qi
    wi = dr * pi - di * pr + er * qi - ei * qr
    scale = -1.0 / (cr * cr + ci * ci)
    kr, ki = (wr * cr - wi * ci) * scale, (wr * ci + wi * cr) * scale
    second = []
    for k, p, q in ((kr, pr, qr), (ki, pi, qi)):
        second.append(jnp.stack([choose(masks, k, q, p), choose(masks, p, k, q), choose(masks, q, p, k)]))
    return jnp.stack([ar, second[0]]), jnp.stack([ai, second[1]])


def pair(block):
    half = block.reshape(2, -1, *block.shape[1:])
    return tuple(m.reshape(-1, 3, *block.shape[1:]) for m in half)


def flat(mat):
    return jnp.concatenate([m.reshape(-1, *m.shape[2:]) for m in mat], axis=0)


def join(early, late, sub):
    row = lax.broadcasted_iota(jnp.int32, early.shape, 1) // (ROWS // 2)
    lane = lax.broadcasted_iota(jnp.int32, early.shape, 2) // sub % 2
    early_turned, late_turned = (pltpu.roll(b, ROWS // 2, 1) for b in (early, late))
    even = jnp.where(row == 0, early, late_turned)
    odd = jnp.where(row == 0, early_turned, late)
    return jnp.where(lane == 0, even, odd)


def spread(total, nx, nt, sub, out_ref):
    shape = (nx * nt, LANES)
    corner = lax.broadcasted_iota(jnp.int32, shape, 0)
    column = lax.broadcasted_iota(jnp.int32, shape, 1)
    base = (corner // nt) * (sub * nt) + corner % nt
    for r in range(RMAX):
        first = r * TMAX // sub
        item = jnp.minimum(column + (r * TMAX - first * sub), 2 * sub - 1)
        lanes = base + item % sub * nt
        value = None
        for g in range(first, (r * TMAX + TMAX - 1) // sub + 1):
            line = jnp.broadcast_to(total[g : g + 1], shape)
            line = jnp.take_along_axis(line, lanes, axis=1)
            value = line if value is None else jnp.where(item < sub, value, line)
        out_ref[r] = value.reshape(nx, nt, LANES)[:, :, :TMAX]


def kernel(
    dims, lx_ref, lt_ref, out_ref, raw, first, block, send, recv, lines, edge, middle, step_t, trans, part,
    gath, in_sem, send_sem, recv_sem, send2_sem, recv2_sem, entered,
):
    gx, gy, ta, nx, nt, ns, sub = dims
    groups = gx * ta
    total_t = ta * nt
    mx, my, mt = lax.axis_index("gx"), lax.axis_index("gy"), lax.axis_index("ta")
    me = mt * gx + mx
    sites = nx * nt
    comps = 12
    short = 10

    inner = lax.rem((mt + 1) // 2, 2)
    opposite, second = ta - 1 - mt, lax.rem(mt + 2, ta)
    ranks = [
        mt,
        mt + 1 - 2 * lax.rem(mt, 2),
        inner * opposite + (1 - inner) * second,
        inner * second + (1 - inner) * opposite,
    ]
    steps = [(a, b, c, d) for a in range(2) for b in range(2) for c in range(gy) for d in range(ta)]
    steps = [o for o in steps if any(o)]
    plane = [o for o in steps if o[2] == 0]
    plane.sort(key=lambda o: (-o[3] * 2 - o[0] * 3, o[1]))
    steps.sort(key=lambda o: (-o[2] - o[0] - o[3], o[1]))
    peers = [o for o in steps if o[0] == o[1] == o[3] == 0]

    def target(step):
        a, b, c, d = step
        return {
            "gx": lax.rem(mx // 2 + a, 2) * 2 + lax.rem(mx + b, 2),
            "gy": lax.rem(my + c, gy),
            "ta": ranks[d],
        }

    barrier = pltpu.get_barrier_semaphore()
    for step in plane + peers:
        pl.semaphore_signal(barrier, inc=1, device_id=target(step), device_id_type=MESH)

    for f, ref in enumerate((lt_ref, lx_ref)):
        for c in range(2):
            pltpu.make_async_copy(
                ref.at[c, pl.ds(0, 6 * sites)], raw.at[f, pl.ds(c * 6 * sites, 6 * sites)], in_sem.at[f]
            ).start()

    with scope("p_load"):
        pltpu.make_async_copy(raw.at[0], raw.at[0], in_sem.at[0]).wait()
    with scope("p_local"):
        t_local = lax.broadcasted_iota(jnp.int32, (sites, LANES), 0) % nt
        x_local = lax.broadcasted_iota(jnp.int32, (sites, LANES), 0) // nt
        line = pair(raw[0].reshape(comps, sites, LANES))
        step = 1
        while step < nt:
            earlier = unit_where(t_local >= step, rolled(line, step, 1))
            line = product(earlier, full(line))
            step *= 2
        first[...] = flat(line).reshape(comps * sites, LANES)
        for k in range(2):
            for m in range(3):
                for xl in range(2):
                    block[k, pl.ds(short * ROWS + m * ROWS + xl * 4, 4), :] = first[
                        pl.ds(4 * m * sites + (2 * k + xl) * nt + nt - 1, 4, stride=sites), :
                    ]
            for tt in range(2):
                block[k, pl.ds(short * ROWS + 2 * comps + tt * comps, comps), :] = first[
                    pl.ds(2 * k + tt, comps, stride=sites), :
                ]
        gauge = unit_where(t_local >= 1, rolled(line, 1, 1))
        pltpu.make_async_copy(raw.at[1], raw.at[1], in_sem.at[1]).wait()
        link = full(pair(raw[1].reshape(comps, sites, LANES)))
        beyond = unit_where(x_local < nx - 1, rolled(full(gauge), sites - nt, 1))
        parts = shorten(product_dagger(product(gauge, link), beyond))
        for k in range(2):
            for c in range(short):
                block[k, pl.ds(c * ROWS, ROWS), :] = parts[c][k * ROWS : (k + 1) * ROWS]
            send[:, pl.ds(k * sub, sub), :] = block[k].T.reshape(groups, sub, LANES)

    with scope("p_bar"):
        pl.semaphore_wait(barrier, len(plane + peers))
    for step in peers:
        pl.semaphore_signal(entered, inc=1, device_id=target(step), device_id_type=MESH)

    for step in plane:
        where = target(step)
        pltpu.make_async_remote_copy(
            src_ref=send.at[where["ta"] * gx + where["gx"]],
            dst_ref=recv.at[me],
            send_sem=send_sem,
            recv_sem=recv_sem.at[mt // 2],
            device_id=where,
            device_id_type=MESH,
        ).start()
    own = pltpu.make_async_copy(send.at[me], recv.at[me], recv_sem.at[mt // 2])
    own.start()

    def next_x(mat):
        return tuple(
            pltpu.roll(m.reshape(-1, LANES), LANES - sub, 1).reshape(m.shape) for m in mat
        )

    t_half = lax.broadcasted_iota(jnp.int32, (ROWS, LANES), 0) % nt
    x_lane = lax.broadcasted_iota(jnp.int32, (ROWS, LANES), 1) // sub % nx
    for order in range(2):
        half = lax.rem(mt // 2 + order, 2)
        landed = recv.at[pl.ds(half * 2 * gx, 2 * gx)]
        with scope(f"p_w{order}"):
            pltpu.make_async_copy(landed, landed, recv_sem.at[half]).wait()
        with scope(f"p_half{order}"):
            got = recv[pl.ds(half * 2 * gx, 2 * gx)].reshape(2, gx * 2, sub, LANES)
            got = [jnp.stack([got[td], got[td]], axis=1).reshape(LANES, LANES).T for td in range(2)]
            cuts = short * ROWS, short * ROWS + 2 * comps
            parts = join(*(g[: cuts[0]].reshape(short, ROWS, LANES) for g in got), sub)
            ends = join(*(g[cuts[0] : cuts[1]].reshape(3, ROWS, LANES) for g in got), sub)
            for m in range(3):
                for td in range(2):
                    lines[pl.ds(4 * m * ROWS + half * 2 + td + 1, 4, stride=ROWS), :] = ends[m, td * 4 : td * 4 + 4]
            for td in range(2):
                near = pltpu.roll(got[td][cuts[1] :], LANES - sub, 1)
                far = pltpu.roll(got[td][cuts[1] : cuts[1] + 2 * ROWS], LANES - 3 * sub, 1)
                edge[pl.ds(td * nt + 1, comps, stride=ROWS), :] = near[:comps]
                edge[pl.ds(td * nt + 2, comps, stride=ROWS), :] = near[comps:]
                edge[pl.ds(td * nt + 3, comps, stride=ROWS), :] = far[:comps]
            end = pair(edge[...].reshape(comps, ROWS, LANES))
            end = full(unit_where((t_half > 0) & (x_lane == nx - 1), end))
            middle[:, pl.ds(half * ROWS, ROWS), :] = flat(product_dagger(lengthen(parts), end))

    with scope("p_prefix"):
        row = lax.broadcasted_iota(jnp.int32, (ROWS, LANES), 0)
        hop = lines[...].reshape(comps, ROWS, LANES)
        hop = jnp.where(row == ta + 1, pltpu.roll(hop, ta, 1), hop)
        hop = unit_where((row > 0) & (row < ta + 2), pair(hop))
        step = 1
        while step < ta + 2:
            earlier = unit_where(row >= step, rolled(hop, step, 1))
            hop = product(earlier, full(hop))
            step *= 2
        hop = full(hop)
        step_t[0] = flat(hop).reshape(18 * ROWS, LANES)
        step_t[1] = flat(next_x(hop)).reshape(18 * ROWS, LANES)

    def spread_t(side, rows, v):
        out = []
        for c in range(18):
            if c % 9 >= 3 * rows:
                continue
            low, high = (
                jnp.broadcast_to(step_t[side, pl.ds(c * ROWS + 2 * v + td, 1), :], (ROWS, LANES))
                for td in range(2)
            )
            out.append(jnp.where(row < nt, low, high))
        return pair(jnp.stack(out))

    row_t = row // nt
    lane = lax.broadcasted_iota(jnp.int32, (ROWS, LANES), 1)
    block_x = lane // (LANES // nx)
    own_time = row % nt * (LANES // nx) + lane % (LANES // nx)

    def emit(items, g, held):
        stack = []
        for td in range(ta):
            for a, b in zip(items[::2], items[1::2]):
                a, b = a[td // 2], b[td // 2]
                if td % 2:
                    stack.append(jnp.where(row_t == 0, pltpu.roll(a, nt, 0), b))
                else:
                    stack.append(jnp.where(row_t == 0, a, pltpu.roll(b, nt, 0)))
            stack += [jnp.zeros((ROWS, LANES), jnp.float32)] * ((sub - len(items)) // 2)
        turned = jnp.concatenate(stack, axis=0).T.reshape(gx * nx, sub, LANES)
        turned = turned + pltpu.roll(turned, nt, 1)
        if g % 2 == 0 and g < rows - 1:
            return turned
        low = turned if held is None else held
        for j in range(gx):
            value = None
            for x in range(nx):
                both = jnp.where(row_t == 0, low[j * nx + x], turned[j * nx + x])
                for swapped in (row + 2 - row // 2 % 2 * 4, row + 1 - row % 2 * 2):
                    both = both + jnp.take_along_axis(both, swapped, axis=0)
                both = jnp.take_along_axis(both, own_time, axis=1)
                value = both if value is None else jnp.where(block_x == x, both, value)
            for k in range(1 if held is None else 2):
                part[pl.ds(j * ROWS + g // 2 * 2 + k, ta, stride=gx * ROWS), :] = value[k * nt : k * nt + ta]
        return None

    rows = -(-RMAX * TMAX // sub)
    with scope("p_path"):
        for v in range(total_t // ROWS + 1):
            start = v * ROWS
            inner = pair(middle[:, pl.ds(start % total_t, ROWS), :])
            moved = product(spread_t(0, 2, v), full(product_dagger(inner, spread_t(1, 3, v))))
            trans[0, :, pl.ds(start, ROWS), :] = flat(full(moved))
    with scope("p_sums"):
        items, g, held = [], 0, None
        for r in range(RMAX):
            for v in range(total_t // ROWS + 1) if r else ():
                here = pl.ds(v * ROWS, ROWS)
                moved = pair(pltpu.roll(trans[0, :, here, :].reshape(-1, LANES), LANES - r * sub, 1).reshape(18, ROWS, LANES))
                path = pair(trans[r - 1, :, here, :])
                path = product((path[0][:2], path[1][:2]), moved)
                trans[r, :, here, :] = flat(full(path))
            for u in range(1, TMAX + 1):
                items.append(
                    [
                        jnp.sum(trans[r, :, pl.ds(start, ROWS), :] * trans[r, :, pl.ds(start + u, ROWS), :], axis=0)
                        for start in range(0, total_t, ROWS)
                    ]
                )
                if len(items) == sub or (r, u) == (RMAX - 1, TMAX):
                    held = emit(items, g, held)
                    items, g = [], g + 1

    slot = my * groups + me
    with scope("p_entered"):
        pl.semaphore_wait(entered, len(peers))
    with scope("p_send2"):
        for step in steps:
            where = target(step)
            pltpu.make_async_remote_copy(
                src_ref=part.at[pl.ds((where["ta"] * gx + where["gx"]) * ROWS, rows)],
                dst_ref=gath.at[slot],
                send_sem=send2_sem,
                recv_sem=recv2_sem,
                device_id=where,
                device_id_type=MESH,
            ).start()
    gath[slot] = part[pl.ds(me * ROWS, rows), :]
    with scope("p_wait2"):
        sent = send.at[pl.ds(0, len(plane))]
        pltpu.make_async_copy(sent, sent, send_sem).wait()
        landed = gath.at[pl.ds(0, len(steps))]
        pltpu.make_async_copy(landed, landed, send2_sem).wait()
        pltpu.make_async_copy(landed, landed, recv2_sem).wait()
    total = [gath[k] for k in range(gy * groups)]
    while len(total) > 1:
        total = [sum(total[k : k + 2]) for k in range(0, len(total), 2)]
    spread(total[0] * (1.0 / (3.0 * (ns * gy))), nx, nt, sub, out_ref)


def fast(dims, link_x, link_t):
    gx, gy, ta, nx, nt, ns, sub = dims
    groups = gx * ta
    total_t = ta * nt
    flat = (2, 9 * nx * nt, ns)
    rows = -(-RMAX * TMAX // sub)
    out = pl.pallas_call(
        functools.partial(kernel, dims),
        out_shape=pltpu.VMEM((RMAX, nx, nt, TMAX), jnp.float32),
        in_specs=[pl.BlockSpec(memory_space=pl.ANY)] * 2,
        out_specs=pl.BlockSpec(memory_space=pltpu.VMEM),
        scratch_shapes=[
            pltpu.VMEM((2, 12 * nx * nt, ns), jnp.float32),
            pltpu.VMEM((12 * nx * nt, ns), jnp.float32),
            pltpu.VMEM((2, LANES, ns), jnp.float32),
            pltpu.VMEM((groups, 2 * sub, LANES), jnp.float32),
            pltpu.VMEM((groups, 2 * sub, LANES), jnp.float32),
            pltpu.VMEM((12 * ROWS, LANES), jnp.float32),
            pltpu.VMEM((12 * ROWS, LANES), jnp.float32),
            pltpu.VMEM((12, total_t, LANES), jnp.float32),
            pltpu.VMEM((2, 18 * ROWS, LANES), jnp.float32),
            pltpu.VMEM((RMAX, 18, total_t + ROWS, LANES), jnp.float32),
            pltpu.VMEM((groups * ROWS, LANES), jnp.float32),
            pltpu.VMEM((gy * groups, rows, LANES), jnp.float32),
            pltpu.SemaphoreType.DMA((2,)),
            pltpu.SemaphoreType.DMA,
            pltpu.SemaphoreType.DMA((2,)),
            pltpu.SemaphoreType.DMA,
            pltpu.SemaphoreType.DMA,
            pltpu.SemaphoreType.REGULAR,
        ],
        compiler_params=pltpu.CompilerParams(collective_id=0, has_side_effects=True),
        name="wilson",
    )(link_x.reshape(flat), link_t.reshape(flat))
    return out.transpose(0, 3, 1, 2)


def times(left, right):
    def dot(a, b):
        return sum(a[:, j][:, None] * b[j][None] for j in range(3))

    real = dot(left[0], right[0]) - dot(left[1], right[1])
    imag = dot(left[0], right[1]) + dot(left[1], right[0])
    return jnp.stack([real, imag])


def general(dims, link_x, link_t):
    gx, gy, ta, nx, nt, ns, sub = dims

    def gather(field):
        field = lax.all_to_all(field, "gx", 5, 3, tiled=True)
        return lax.all_to_all(field, "ta", 5, 4, tiled=True)

    link_x, link_t = gather(link_x), gather(link_t)

    def grow_t(carry, _):
        line, factor = carry
        factor = jnp.roll(factor, -1, axis=4)
        return (times(line, factor), factor), line

    _, temporal = lax.scan(grow_t, (link_t, link_t), None, length=TMAX)

    def radius(carry, _):
        spatial, factor, carried = carry
        carried = jnp.roll(carried, -1, axis=4)

        def extent(shifted, pair):
            line, line_r = pair
            shifted = jnp.roll(shifted, -1, axis=4)
            return shifted, jnp.sum(times(spatial, line_r) * times(line, shifted), axis=(0, 1, 2, 5))

        _, sums = lax.scan(extent, spatial, (temporal, carried))
        factor = jnp.roll(factor, -1, axis=3)
        return (times(spatial, factor), factor, carried), sums

    _, loops = lax.scan(radius, (link_x, link_x, temporal), None, length=RMAX)
    loops = lax.psum(loops, ("gx", "gy", "ta"))
    loops = lax.dynamic_slice_in_dim(loops, lax.axis_index("gx") * nx, nx, axis=2)
    loops = lax.dynamic_slice_in_dim(loops, lax.axis_index("ta") * nt, nt, axis=3)
    return loops / (3.0 * (ns * gy))


def local(link_x, link_t):
    gx, gy, ta = (lax.axis_size(a) for a in ("gx", "gy", "ta"))
    nx, nt, ns = link_x.shape[3:]
    sub = ns // (gx * ta)
    dims = (gx, gy, ta, nx, nt, ns, sub)
    fits = (
        ns == LANES
        and sub == ROWS
        and gx == nx == nt == ta == 4
    )
    return (fast if fits else general)(dims, link_x, link_t)


def solution(mesh):
    spec = P(None, None, None, "gx", "ta", "gy")
    return jax.shard_map(
        local,
        mesh=mesh,
        in_specs=(spec, spec),
        out_specs=P(None, None, "gx", "ta"),
        check_vma=False,
    )
```
